32 devices in a mesh: case: 1 (over z), model: 4 (over y), ens: 8 (over x, core).
Axes of the slice: x: 4, y: 4, z: 1, core: 2. Of those that a mesh axis runs over, the one named last changes fastest.
The devices are a block of a 4x4x8 slice.
Arguments:
- ens_init: float32 [32, 5120, 64], P(('case', 'ens'), None, 'model')
- mix_op: bfloat16 [5120, 5120], replicated
- w_in: bfloat16 [3, 64, 1024], P(None, None, 'model')
- w_out: bfloat16 [3, 1024, 64], P(None, 'model')
- obs_val: float32 [2, 5120, 32], P(None, ('case', 'ens', 'model'))
- obs_prec: float32 [5120, 32], P(('case', 'ens', 'model'))
- obs_idx: int32 [32], replicated
- inflation: float32 [1], replicated
Outputs:
- output: float32 [32, 5120, 64], P(('case', 'ens'), None, 'model')
All inputs are finite; a program needn't handle non-finite values.
Results may differ from the reference program's by a relative error of at most 0.0131299.
Values are sent between devices in bfloat16 or wider.
A program may use at most 768 MiB of HBM per device.

```python
import jax
import jax.numpy as jnp
from jax import lax

COLS = 5120
VARS = 64
HIDDEN = 1024
OBS_VARS = 32
LAYERS = 3
CYCLES = 2
MEMBERS = 32
NS_STEPS = 12
COL_BLOCK = 160


def setup_inputs(seed: int = 0, part: int = 0) -> dict:
    shared_keys = jax.random.split(jax.random.key(seed), 5)
    part_keys = jax.random.split(jax.random.fold_in(jax.random.key(seed + 1), part), 4)
    base_state = jax.random.normal(part_keys[0], (COLS, VARS), jnp.float32)
    spread = jax.random.normal(part_keys[1], (MEMBERS, COLS, VARS), jnp.float32)
    ens_init = base_state[None] + 0.4 * spread
    obs_val = jax.random.normal(part_keys[2], (CYCLES, COLS, OBS_VARS), jnp.float32)
    obs_prec = jax.random.uniform(part_keys[3], (COLS, OBS_VARS), jnp.float32, 0.75, 5.25)
    mix_op = (jax.random.normal(shared_keys[0], (COLS, COLS), jnp.float32) * COLS ** -0.5).astype(jnp.bfloat16)
    w_in = (jax.random.normal(shared_keys[1], (LAYERS, VARS, HIDDEN), jnp.float32) * VARS ** -0.5).astype(jnp.bfloat16)
    w_out = (jax.random.normal(shared_keys[2], (LAYERS, HIDDEN, VARS), jnp.float32) * (0.5 * HIDDEN ** -0.5)).astype(jnp.bfloat16)
    obs_idx = jax.random.permutation(shared_keys[3], VARS)[:OBS_VARS].astype(jnp.int32)
    inflation = jax.random.uniform(shared_keys[4], (1,), jnp.float32, 1.0, 1.6)
    return dict(ens_init=ens_init, mix_op=mix_op, w_in=w_in, w_out=w_out, obs_val=obs_val, obs_prec=obs_prec, obs_idx=obs_idx, inflation=inflation)


def forecast_member(member, mix_op, w_in, w_out):
    def layer_step(state_now, weights):
        w_first, w_second = weights
        mix_out = jnp.dot(mix_op, state_now.astype(jnp.bfloat16), preferred_element_type=jnp.float32).astype(jnp.bfloat16)
        hidden = jax.nn.gelu(jnp.dot(mix_out, w_first, preferred_element_type=jnp.float32), approximate=True)
        update = jnp.dot(hidden.astype(jnp.bfloat16), w_second, preferred_element_type=jnp.float32)
        return state_now + update, None
    result, unused = lax.scan(layer_step, member, (w_in, w_out))
    return result


def analyse_block(col_block, obs_now, prec_now, obs_idx, inflation):
    ens_mean = jnp.mean(col_block, axis=1)
    anomaly = col_block - ens_mean[:, None, :]
    obs_anom = jnp.take(anomaly, obs_idx, axis=2)
    innovation = obs_now - jnp.take(ens_mean, obs_idx, axis=1)
    weighted = obs_anom * prec_now[:, None, :]
    identity = jnp.eye(MEMBERS, dtype=jnp.float32)
    a_tilde = ((MEMBERS - 1) / inflation[0]) * identity + jnp.einsum('bip,bjp->bij', weighted, obs_anom)
    trace_sum = jnp.trace(a_tilde, axis1=1, axis2=2)[:, None, None]
    b_mat = a_tilde / trace_sum
    z_mat = jnp.broadcast_to(identity, a_tilde.shape)
    for ns_step in range(NS_STEPS):
        t_mat = 1.5 * identity - 0.5 * jnp.einsum('bij,bjk->bik', z_mat, b_mat)
        b_mat = jnp.einsum('bij,bjk->bik', b_mat, t_mat)
        z_mat = jnp.einsum('bij,bjk->bik', t_mat, z_mat)
    sqrt_inv = z_mat / jnp.sqrt(trace_sum)
    gain_vec = jnp.einsum('bip,bp->bi', weighted, innovation)
    half_step = jnp.einsum('bij,bj->bi', sqrt_inv, gain_vec)
    w_mean = jnp.einsum('bij,bj->bi', sqrt_inv, half_step)
    w_full = (MEMBERS - 1) ** 0.5 * sqrt_inv + w_mean[:, :, None]
    return ens_mean[:, None, :] + jnp.einsum('bik,biv->bkv', w_full, anomaly)


def reference(ens_init, mix_op, w_in, w_out, obs_val, obs_prec, obs_idx, inflation):
    n_blocks = COLS // COL_BLOCK
    prec_blocks = obs_prec.reshape(n_blocks, COL_BLOCK, OBS_VARS)

    def forecast_one(member):
        return forecast_member(member, mix_op, w_in, w_out)

    def analyse_pieces(pieces):
        return analyse_block(pieces[0], pieces[1], pieces[2], obs_idx, inflation)

    def run_cycle(ens_state, obs_now):
        ens_state = lax.map(forecast_one, ens_state)
        col_blocks = ens_state.reshape(MEMBERS, n_blocks, COL_BLOCK, VARS).transpose(1, 2, 0, 3)
        obs_blocks = obs_now.reshape(n_blocks, COL_BLOCK, OBS_VARS)
        analysed = lax.map(analyse_pieces, (col_blocks, obs_blocks, prec_blocks))
        return analysed.transpose(2, 0, 1, 3).reshape(MEMBERS, COLS, VARS), None

    final_state, unused = lax.scan(run_cycle, ens_init, obs_val)
    return final_state
```

```python
import functools

import jax
import jax.numpy as jnp
from jax import lax
from jax.experimental import pallas as pl
from jax.experimental.pallas import tpu as pltpu
from jax.sharding import PartitionSpec as P

NS_STEPS = 12
LANES = 128
SUB = 8
MESH = pl.DeviceIdType.MESH
VMEM = pl.BlockSpec(memory_space=pltpu.VMEM)
SMEM = pl.BlockSpec(memory_space=pltpu.SMEM)


def greet(peers):
    barrier = pltpu.get_barrier_semaphore()
    for peer in peers:
        pl.semaphore_signal(barrier, inc=1, device_id=peer, device_id_type=MESH)
    pl.semaphore_wait(barrier, len(peers))


def gather_vars_kernel(n_model, x_ref, w_ref, u_ref, h_ref, wa_ref, ua_ref, send_sem, recv_sem, own_sem):
    me = lax.axis_index('model')
    others = [lax.rem(me + t, n_model) for t in range(1, n_model)]
    greet([{'model': o} for o in others])
    copies = []
    for t, o in enumerate(others):
        for a, (src, dst) in enumerate(((x_ref.at[o], h_ref.at[me]), (w_ref, wa_ref.at[me]), (u_ref, ua_ref.at[me]))):
            copies.append(pltpu.make_async_remote_copy(src_ref=src, dst_ref=dst, send_sem=send_sem.at[3 * t + a], recv_sem=recv_sem.at[3 * t + a], device_id={'model': o}, device_id_type=MESH))
    for copy in copies:
        copy.start()
    own = [pltpu.make_async_copy(src, dst, own_sem.at[a]) for a, (src, dst) in enumerate(((x_ref.at[me], h_ref.at[me]), (w_ref, wa_ref.at[me]), (u_ref, ua_ref.at[me])))]
    for copy in own:
        copy.start()
    for copy in own + copies:
        copy.wait()


def gather_vars(x, w, u, n_model):
    n_sem = 3 * (n_model - 1)
    return pl.pallas_call(
        functools.partial(gather_vars_kernel, n_model),
        out_shape=(jax.ShapeDtypeStruct(x.shape, x.dtype), jax.ShapeDtypeStruct((n_model,) + w.shape, w.dtype), jax.ShapeDtypeStruct((n_model,) + u.shape, u.dtype)),
        in_specs=[VMEM] * 3,
        out_specs=[VMEM] * 3,
        scratch_shapes=[pltpu.SemaphoreType.DMA((n_sem,)), pltpu.SemaphoreType.DMA((n_sem,)), pltpu.SemaphoreType.DMA((3,))],
        compiler_params=pltpu.CompilerParams(collective_id=0, has_side_effects=True),
        name='gather_vars',
    )(x, w, u)


def exchange_kernel(n_model, n_ens, x_ref, o_ref, send_sem, recv_sem, own_sem):
    my_m, my_e = lax.axis_index('model'), lax.axis_index('ens')
    me = my_e * n_model + my_m
    steps = [(e, m) for e in range(n_ens) for m in range(n_model)][1:]
    peers = [(lax.rem(my_e + e, n_ens), lax.rem(my_m + m, n_model)) for e, m in steps]
    greet([{'ens': e, 'model': m} for e, m in peers])
    copies = []
    for t, (e, m) in enumerate(peers):
        copies.append(pltpu.make_async_remote_copy(src_ref=x_ref.at[e * n_model + m], dst_ref=o_ref.at[me], send_sem=send_sem.at[t], recv_sem=recv_sem.at[t], device_id={'ens': e, 'model': m}, device_id_type=MESH))
    for copy in copies:
        copy.start()
    own = pltpu.make_async_copy(x_ref.at[me], o_ref.at[me], own_sem)
    own.start()
    own.wait()
    for copy in copies:
        copy.wait()


def exchange(x, n_model, n_ens):
    n_sem = n_model * n_ens - 1
    return pl.pallas_call(
        functools.partial(exchange_kernel, n_model, n_ens),
        out_shape=jax.ShapeDtypeStruct(x.shape, x.dtype),
        in_specs=[VMEM],
        out_specs=VMEM,
        scratch_shapes=[pltpu.SemaphoreType.DMA((n_sem,)), pltpu.SemaphoreType.DMA((n_sem,)), pltpu.SemaphoreType.DMA],
        compiler_params=pltpu.CompilerParams(collective_id=1, has_side_effects=True),
        name='exchange',
    )(x)


GELU_C = 0.7978845608028654


def layer_kernel(hb_ref, h_ref, a_ref, wt_ref, ut_ref, ho_ref, hbo_ref):
    mix = lax.dot_general(hb_ref[...], a_ref[...], (((1,), (1,)), ((), ())), preferred_element_type=jnp.float32).astype(jnp.bfloat16)
    half = jnp.dot(wt_ref[...], mix, preferred_element_type=jnp.float32)
    arg = half * (2 * GELU_C + (8 * GELU_C * 0.044715) * (half * half))
    act = half * jnp.tanh(arg) + half
    new = h_ref[...] + jnp.dot(ut_ref[...], act.astype(jnp.bfloat16), preferred_element_type=jnp.float32)
    ho_ref[...] = new
    hbo_ref[...] = new.astype(jnp.bfloat16)


def layer(hb, h, mix_op, wt, ut, block=256):
    n_vars, cols = h.shape
    hidden = wt.shape[0]
    return pl.pallas_call(
        layer_kernel,
        grid=(cols // block,),
        out_shape=(jax.ShapeDtypeStruct(h.shape, jnp.float32), jax.ShapeDtypeStruct(h.shape, jnp.bfloat16)),
        in_specs=[
            pl.BlockSpec((n_vars, cols), lambda i: (0, 0)),
            pl.BlockSpec((n_vars, block), lambda i: (0, i)),
            pl.BlockSpec((block, cols), lambda i: (i, 0)),
            pl.BlockSpec((hidden, n_vars), lambda i: (0, 0)),
            pl.BlockSpec((n_vars, hidden), lambda i: (0, 0)),
        ],
        out_specs=(pl.BlockSpec((n_vars, block), lambda i: (0, i)), pl.BlockSpec((n_vars, block), lambda i: (0, i))),
        cost_estimate=pl.CostEstimate(flops=2 * n_vars * cols * (cols + 2 * hidden), bytes_accessed=2 * cols * cols, transcendentals=hidden * cols),
        name='layer',
    )(hb, h, mix_op, wt, ut)


def lane_pick(lanes, pieces):
    out = pieces[-1][1]
    for bound, piece in reversed(pieces[:-1]):
        out = jnp.where(lanes < bound, piece, out)
    return out


def pack_kernel(rem, h_ref, o_ref):
    fold = LANES // rem
    rows = h_ref.shape[0]
    deep = rows // fold
    span = fold * (LANES + rem)
    lanes = lax.broadcasted_iota(jnp.int32, (rows, LANES), 1)
    dlanes = lax.broadcasted_iota(jnp.int32, (deep, LANES), 1)

    @pl.loop(0, h_ref.shape[1] // span)
    def _(a):
        part = [h_ref[:, pl.ds(pl.multiple_of(a * span + g * LANES, LANES), LANES)] for g in range(fold + 1)]
        for b in range(fold):
            j = a * fold + b
            main = part[0] if b == 0 else pltpu.roll(jnp.where(lanes < rem * b, part[b + 1], part[b]), LANES - rem * b, 1)
            o_ref[j, 0:rows, :] = main
            tail = [part[b + 1][deep * q:deep * (q + 1)] for q in range(fold)]
            tail = [x if q == b else pltpu.roll(x, (rem * (q - b)) % LANES, 1) for q, x in enumerate(tail)]
            o_ref[j, rows:rows + deep, :] = lane_pick(dlanes, [(rem * (q + 1), x) for q, x in enumerate(tail)])


def pack(h, n_blocks):
    rows, cols = h.shape
    rem = cols // n_blocks - LANES
    return pl.pallas_call(
        functools.partial(pack_kernel, rem),
        out_shape=jax.ShapeDtypeStruct((n_blocks, rows + rows * rem // LANES, LANES), h.dtype),
        in_specs=[VMEM],
        out_specs=VMEM,
        name='pack',
    )(h)


def unpack_kernel(rem, rows, x_ref, *outs):
    fold = LANES // rem
    deep = rows // fold
    span = fold * (LANES + rem)
    lanes = lax.broadcasted_iota(jnp.int32, (rows, LANES), 1)

    @pl.loop(0, x_ref.shape[0] // fold)
    def _(a):
        mains, tails = [], []
        for b in range(fold):
            main = x_ref[a * fold + b, 0:rows, :]
            mains.append(main if b == 0 else pltpu.roll(main, rem * b, 1))
            tail = x_ref[a * fold + b, rows:rows + deep, :]
            tails.append(jnp.concatenate([tail if q == b else pltpu.roll(tail, (rem * (b - q)) % LANES, 1) for q in range(fold)], axis=0))
        for g in range(fold + 1):
            if g == 0:
                piece = mains[0]
            else:
                piece = jnp.where(lanes < rem * (g - 1), mains[g - 1], tails[g - 1])
                if g < fold:
                    piece = jnp.where(lanes < rem * g, piece, mains[g])
            for out in outs:
                out[:, pl.ds(pl.multiple_of(a * span + g * LANES, LANES), LANES)] = piece.astype(out.dtype)


def unpack(x, rows, dtypes):
    n_blocks, depth, _ = x.shape
    rem = (depth - rows) * LANES // rows
    return pl.pallas_call(
        functools.partial(unpack_kernel, rem, rows),
        out_shape=tuple(jax.ShapeDtypeStruct((rows, n_blocks * (LANES + rem)), t) for t in dtypes),
        in_specs=[VMEM],
        out_specs=tuple(VMEM for t in dtypes),
        name='unpack',
    )(x)


def analysis_kernel(n_model, by_output, idx_ref, rho_ref, x_ref, y_ref, r_ref, o_ref, xs, xa, mean, mats, yo, gy, vec):
    members, depth, _ = x_ref.shape
    n_vars = mean.shape[0]
    n_obs = y_ref.shape[1]
    rem = (depth - n_vars) * LANES // n_vars
    fold = LANES // rem
    deep = n_vars // fold
    groups = members // SUB
    size = members * members
    part = pl.program_id(0)
    eight = lax.broadcasted_iota(jnp.int32, (SUB, LANES), 0)
    dlanes = lax.broadcasted_iota(jnp.int32, (deep, LANES), 1)

    @pl.when(part == 0)
    def _():
        @pl.loop(0, members)
        def _(k):
            xs[pl.ds(pl.multiple_of(k * n_vars, SUB), n_vars), :] = x_ref[k, 0:n_vars, :]

    @pl.when(part != 0)
    def _():
        @pl.loop(0, members)
        def _(k):
            tail = x_ref[k, n_vars:depth, :]
            for q in range(fold):
                xs[pl.ds(pl.multiple_of(k * n_vars + deep * q, SUB), deep), :] = tail if q == 0 else pltpu.roll(tail, LANES - rem * q, 1)

    total = xs[0:n_vars, :]
    for k in range(1, members):
        total = total + xs[k * n_vars:(k + 1) * n_vars, :]
    mean[...] = total * (1.0 / members)

    @pl.loop(0, n_vars)
    def _(v):
        xa[pl.ds(pl.multiple_of(v * members, SUB), members), :] = xs[pl.ds(v, members, stride=n_vars), :] - mean[pl.ds(v, 1), :]

    @pl.loop(0, n_obs)
    def _(p):
        var = idx_ref[p]
        row = pl.multiple_of(p * members, SUB)
        here = xa[pl.ds(pl.multiple_of(var * members, SUB), members), :]
        yo[pl.ds(row, members), :] = here
        gy[pl.ds(row, members), :] = here * r_ref[0, pl.ds(p, 1), :]
        vec[pl.ds(p, 1), :] = y_ref[0, pl.ds(p, 1), :] - mean[pl.ds(var, 1), :]

    def product(left, left_at, right, right_at, out, out_at, scale, diag):
        for i in range(groups):
            wide = members - SUB * i

            def body(kk, acc):
                for k4 in range(4):
                    k = (kk * 4 + k4) * members + SUB * i
                    r = right[pl.ds(pl.multiple_of(right_at + k, SUB), wide), :]
                    acc = tuple(acc[a] + left[pl.ds(left_at + k + a, 1), :] * r for a in range(SUB))
                return acc

            acc = lax.fori_loop(0, members // 4, body, tuple(jnp.zeros((wide, LANES), jnp.float32) for a in range(SUB)))
            for a in range(SUB):
                val = acc[a] if scale is None else acc[a] * scale
                first = val[0:SUB]
                if diag is not None:
                    first = first + jnp.where(eight == a, diag, 0.0)
                out[pl.ds(pl.multiple_of(out_at + (SUB * i + a) * members + SUB * i, SUB), SUB), :] = first
                if i + 1 < groups:
                    out[pl.ds(pl.multiple_of(out_at + (SUB * i + a) * members + SUB * (i + 1), SUB), wide - SUB), :] = val[SUB:]
                    out[pl.ds(out_at + SUB * (i + 1) * members + SUB * i + a, wide - SUB, stride=members), :] = val[SUB:]

    slot = lambda s: pl.multiple_of(lax.rem(s + 4 * NS_STEPS, 4) * size, SUB)
    product(gy, 0, yo, 0, mats, slot(3), None, (members - 1) / rho_ref[0])
    trace = jnp.sum(mats[pl.ds(slot(3), members, stride=members + 1), :], axis=0, keepdims=True)
    inv = 1.0 / trace

    @pl.loop(0, members)
    def _(i):
        row = pl.multiple_of(i * members, SUB)
        b = mats[pl.ds(slot(3) + row, members), :] * inv
        eye = jnp.where(lax.broadcasted_iota(jnp.int32, (members, LANES), 0) == i, 1.5, 0.0)
        t = eye - 0.5 * b
        mats[pl.ds(slot(0) + row, members), :] = b
        mats[pl.ds(slot(1) + row, members), :] = t
        mats[pl.ds(slot(2) + row, members), :] = t

    def step(s, carry):
        b, t, z, n = slot(-s), slot(1 - s), slot(2 - s), slot(3 - s)
        product(mats, b, mats, t, mats, n, None, None)
        product(mats, z, mats, n, mats, b, -0.5, 1.5)
        product(mats, b, mats, z, mats, t, None, None)
        return carry

    lax.fori_loop(0, NS_STEPS - 1, step, 0)
    z = slot(2 - (NS_STEPS - 1))
    root = 1.0 / jnp.sqrt(trace)

    def weighted(left, at, base, scale):
        acc = jnp.zeros((members, LANES), jnp.float32)
        for p in range(left.shape[0] // members if left is not mats else members):
            acc = acc + left[pl.ds(at + p * members, members), :] * vec[base + p:base + p + 1, :]
        return acc if scale is None else acc * scale

    vec[n_obs:n_obs + members, :] = weighted(gy, 0, 0, None)
    vec[n_obs + members:n_obs + 2 * members, :] = weighted(mats, z, n_obs, root)
    vec[n_obs:n_obs + members, :] = weighted(mats, z, n_obs + members, root)

    @pl.loop(0, members)
    def _(i):
        row = pl.multiple_of(i * members, SUB)
        gy[pl.ds(row, members), :] = mats[pl.ds(z + row, members), :] * (root * (members - 1) ** 0.5) + vec[pl.ds(n_obs + i, 1), :]

    @pl.loop(0, n_vars // 4)
    def _(v4):
        acc = [jnp.broadcast_to(mean[pl.ds(v4 * 4 + c, 1), :], (members, LANES)) for c in range(4)]

        def body(ii, acc):
            for i4 in range(4):
                i = ii * 4 + i4
                wa = gy[pl.ds(pl.multiple_of(i * members, SUB), members), :]
                acc = tuple(acc[c] + xa[pl.ds((v4 * 4 + c) * members + i, 1), :] * wa for c in range(4))
            return acc

        acc = lax.fori_loop(0, members // 4, body, tuple(acc))
        for c in range(4):
            xs[pl.ds(v4 * 4 + c, members, stride=n_vars), :] = acc[c]

    def source(dest, q):
        if by_output:
            return pl.multiple_of((dest // n_model * n_model + q) * n_vars + dest % n_model * deep, SUB)
        return pl.multiple_of(dest * n_vars + q * deep, SUB)

    @pl.when(part == 0)
    def _():
        @pl.loop(0, members)
        def _(dest):
            for q in range(fold):
                o_ref[dest, deep * q:deep * (q + 1), :] = xs[pl.ds(source(dest, q), deep), :]

    @pl.when(part != 0)
    def _():
        @pl.loop(0, members)
        def _(dest):
            tail = [xs[pl.ds(source(dest, q), deep), :] for q in range(fold)]
            tail = [x if q == 0 else pltpu.roll(x, rem * q, 1) for q, x in enumerate(tail)]
            o_ref[dest, n_vars:depth, :] = lane_pick(dlanes, [(rem * (q + 1), x) for q, x in enumerate(tail)])


def analysis(x, y, r, obs_idx, inflation, n_vars, n_model, by_output):
    members, depth, _ = x.shape
    parts, n_obs, _ = y.shape
    whole = pl.BlockSpec(x.shape, lambda g: (0, 0, 0))
    obs = pl.BlockSpec((1, n_obs, LANES), lambda g: (g, 0, 0))
    return pl.pallas_call(
        functools.partial(analysis_kernel, n_model, by_output),
        grid=(parts,),
        out_shape=jax.ShapeDtypeStruct(x.shape, jnp.float32),
        in_specs=[SMEM, SMEM, whole, obs, obs],
        out_specs=whole,
        scratch_shapes=[
            pltpu.VMEM((members * n_vars, LANES), jnp.float32),
            pltpu.VMEM((members * n_vars, LANES), jnp.float32),
            pltpu.VMEM((n_vars, LANES), jnp.float32),
            pltpu.VMEM((4 * members * members, LANES), jnp.float32),
            pltpu.VMEM((n_obs * members, LANES), jnp.float32),
            pltpu.VMEM((n_obs * members, LANES), jnp.float32),
            pltpu.VMEM((n_obs + 2 * members, LANES), jnp.float32),
        ],
        name='analysis',
    )(obs_idx, inflation, x, y, r)


def by_lanes(x, fill):
    x = jnp.swapaxes(x, -1, -2)
    pad = -x.shape[-1] % LANES
    x = jnp.pad(x, [(0, 0)] * (x.ndim - 1) + [(0, pad)], constant_values=fill)
    return jnp.moveaxis(x.reshape(x.shape[:-1] + (-1, LANES)), -2, -3)


def solution(mesh):
    n_model, n_ens = mesh.shape['model'], mesh.shape['ens']

    def local_step(ens_local, mix_op, w_in, w_out, obs_val, obs_prec, obs_idx, inflation):
        held, cols, own_vars = ens_local.shape
        n_blocks = n_model * n_ens
        cycles, layers, n_vars = obs_val.shape[0], w_in.shape[0], w_in.shape[1]
        x = jnp.swapaxes(ens_local, 1, 2)
        h, w_all, u_all = gather_vars(x, w_in, jnp.swapaxes(w_out, 1, 2), n_model)
        h = h.reshape(n_vars, cols)
        hb = h.astype(jnp.bfloat16)
        wt = (jnp.transpose(w_all, (1, 0, 3, 2)) * jnp.bfloat16(0.5)).reshape(layers, -1, n_vars)
        ut = jnp.transpose(u_all, (1, 2, 0, 3)).reshape(layers, n_vars, -1)
        y = by_lanes(obs_val, 0.0)
        r = by_lanes(obs_prec, 1.0)
        for cycle in range(cycles):
            last = cycle + 1 == cycles
            for n in range(layers):
                h, hb = layer(hb, h, mix_op, wt[n], ut[n])
            x = exchange(pack(h, n_blocks), n_model, n_ens)
            x = analysis(x, y[cycle], r, obs_idx, inflation, n_vars, n_model, last)
            x = exchange(x, n_model, n_ens)
            if last:
                (h,) = unpack(x, n_vars, (jnp.float32,))
            else:
                h, hb = unpack(x, n_vars, (jnp.float32, jnp.bfloat16))
        return jnp.swapaxes(h.reshape(held, own_vars, cols), 1, 2)

    member_spec = P(('case', 'ens'), None, 'model')
    col_axes = ('case', 'ens', 'model')
    in_specs = (member_spec, P(None, None), P(None, None, 'model'), P(None, 'model', None), P(None, col_axes, None), P(col_axes, None), P(None), P(None))
    return jax.shard_map(local_step, mesh=mesh, in_specs=in_specs, out_specs=member_spec, check_vma=False)
```

```python
import functools

import jax
import jax.numpy as jnp
from jax import lax
from jax.experimental import pallas as pl
from jax.experimental.pallas import tpu as pltpu
from jax.sharding import PartitionSpec as P

NS_STEPS = 12
PASSES = ((0,), (1,), (2, 3))
LANES = 128
BLOCK = 256
VMEM_LIMIT = 66_500_000
GELU_C = 0.7978845608028654
SUB = 8
MESH = pl.DeviceIdType.MESH
VMEM = pl.BlockSpec(memory_space=pltpu.VMEM)
SMEM = pl.BlockSpec(memory_space=pltpu.SMEM)


def greet(peers):
    barrier = pltpu.get_barrier_semaphore()
    for peer in peers:
        pl.semaphore_signal(barrier, inc=1, device_id=peer, device_id_type=MESH)
    pl.semaphore_wait(barrier, len(peers))


def gather_vars_kernel(n_model, x_ref, w_ref, u_ref, h_ref, wa_ref, ua_ref, send_sem, recv_sem, own_sem):
    me = lax.axis_index('model')
    others = [lax.rem(me + t, n_model) for t in range(1, n_model)]
    greet([{'model': o} for o in others])
    copies = []
    for t, o in enumerate(others):
        for a, (src, dst) in enumerate(((x_ref.at[o], h_ref.at[me]), (w_ref, wa_ref.at[me]), (u_ref, ua_ref.at[me]))):
            copies.append(pltpu.make_async_remote_copy(src_ref=src, dst_ref=dst, send_sem=send_sem.at[3 * t + a], recv_sem=recv_sem.at[3 * t + a], device_id={'model': o}, device_id_type=MESH))
    for copy in copies:
        copy.start()
    own = [pltpu.make_async_copy(src, dst, own_sem.at[a]) for a, (src, dst) in enumerate(((x_ref.at[me], h_ref.at[me]), (w_ref, wa_ref.at[me]), (u_ref, ua_ref.at[me])))]
    for copy in own:
        copy.start()
    for copy in own + copies:
        copy.wait()


def gather_vars(x, w, u, n_model):
    n_sem = 3 * (n_model - 1)
    return pl.pallas_call(
        functools.partial(gather_vars_kernel, n_model),
        out_shape=(jax.ShapeDtypeStruct(x.shape, x.dtype), jax.ShapeDtypeStruct((n_model,) + w.shape, w.dtype), jax.ShapeDtypeStruct((n_model,) + u.shape, u.dtype)),
        in_specs=[VMEM] * 3,
        out_specs=[VMEM] * 3,
        scratch_shapes=[pltpu.SemaphoreType.DMA((n_sem,)), pltpu.SemaphoreType.DMA((n_sem,)), pltpu.SemaphoreType.DMA((3,))],
        compiler_params=pltpu.CompilerParams(collective_id=0, has_side_effects=True),
        name='gather_vars',
    )(x, w, u)


def exchange_kernel(n_model, n_ens, x_ref, o_ref, send_sem, recv_sem, own_sem):
    my_m, my_e = lax.axis_index('model'), lax.axis_index('ens')
    me = my_e * n_model + my_m
    steps = [(e, m) for e in range(n_ens) for m in range(n_model)][1:]
    peers = [(lax.rem(my_e + e, n_ens), lax.rem(my_m + m, n_model)) for e, m in steps]
    greet([{'ens': e, 'model': m} for e, m in peers])
    copies = []
    for t, (e, m) in enumerate(peers):
        copies.append(pltpu.make_async_remote_copy(src_ref=x_ref.at[e * n_model + m], dst_ref=o_ref.at[me], send_sem=send_sem.at[t], recv_sem=recv_sem.at[t], device_id={'ens': e, 'model': m}, device_id_type=MESH))
    for copy in copies:
        copy.start()
    own = pltpu.make_async_copy(x_ref.at[me], o_ref.at[me], own_sem)
    own.start()
    own.wait()
    for copy in copies:
        copy.wait()


def exchange(x, n_model, n_ens):
    n_sem = n_model * n_ens - 1
    return pl.pallas_call(
        functools.partial(exchange_kernel, n_model, n_ens),
        out_shape=jax.ShapeDtypeStruct(x.shape, x.dtype),
        in_specs=[VMEM],
        out_specs=VMEM,
        scratch_shapes=[pltpu.SemaphoreType.DMA((n_sem,)), pltpu.SemaphoreType.DMA((n_sem,)), pltpu.SemaphoreType.DMA],
        compiler_params=pltpu.CompilerParams(collective_id=1, has_side_effects=True),
        name='exchange',
    )(x)


def lane_pick(lanes, pieces):
    out = pieces[-1][1]
    for bound, piece in reversed(pieces[:-1]):
        out = jnp.where(lanes < bound, piece, out)
    return out


def pack_kernel(rem, h_ref, o_ref):
    fold = LANES // rem
    rows = h_ref.shape[0]
    deep = rows // fold
    span = fold * (LANES + rem)
    lanes = lax.broadcasted_iota(jnp.int32, (rows, LANES), 1)
    dlanes = lax.broadcasted_iota(jnp.int32, (deep, LANES), 1)

    @pl.loop(0, h_ref.shape[1] // span)
    def _(a):
        part = [h_ref[:, pl.ds(pl.multiple_of(a * span + g * LANES, LANES), LANES)] for g in range(fold + 1)]
        for b in range(fold):
            j = a * fold + b
            main = part[0] if b == 0 else pltpu.roll(jnp.where(lanes < rem * b, part[b + 1], part[b]), LANES - rem * b, 1)
            o_ref[j, 0:rows, :] = main
            tail = [part[b + 1][deep * q:deep * (q + 1)] for q in range(fold)]
            tail = [x if q == b else pltpu.roll(x, (rem * (q - b)) % LANES, 1) for q, x in enumerate(tail)]
            o_ref[j, rows:rows + deep, :] = lane_pick(dlanes, [(rem * (q + 1), x) for q, x in enumerate(tail)])


def unpack_kernel(rem, rows, x_ref, *outs):
    fold = LANES // rem
    deep = rows // fold
    span = fold * (LANES + rem)
    lanes = lax.broadcasted_iota(jnp.int32, (rows, LANES), 1)

    @pl.loop(0, x_ref.shape[0] // fold)
    def _(a):
        mains, tails = [], []
        for b in range(fold):
            main = x_ref[a * fold + b, 0:rows, :]
            mains.append(main if b == 0 else pltpu.roll(main, rem * b, 1))
            tail = x_ref[a * fold + b, rows:rows + deep, :]
            tails.append(jnp.concatenate([tail if q == b else pltpu.roll(tail, (rem * (b - q)) % LANES, 1) for q in range(fold)], axis=0))
        for g in range(fold + 1):
            if g == 0:
                piece = mains[0]
            else:
                piece = jnp.where(lanes < rem * (g - 1), mains[g - 1], tails[g - 1])
                if g < fold:
                    piece = jnp.where(lanes < rem * g, piece, mains[g])
            for out in outs:
                out[:, pl.ds(pl.multiple_of(a * span + g * LANES, LANES), LANES)] = piece.astype(out.dtype)


def unpack(x, rows, dtypes):
    n_blocks, depth, _ = x.shape
    rem = (depth - rows) * LANES // rows
    return pl.pallas_call(
        functools.partial(unpack_kernel, rem, rows),
        out_shape=tuple(jax.ShapeDtypeStruct((rows, n_blocks * (LANES + rem)), t) for t in dtypes),
        in_specs=[VMEM],
        out_specs=tuple(VMEM for t in dtypes),
        name='unpack',
    )(x)


def forecast_kernel(rem, packed, block, x_ref, a_ref, wt_ref, ut_ref, o_ref, a_all, h, hb, a_sem):
    layers = wt_ref.shape[0]
    n_vars, cols = h.shape
    blocks = cols // block

    def fetch(i):
        rows = pl.ds(pl.multiple_of(i * block, block), block)
        return pltpu.make_async_copy(a_ref.at[rows, :], a_all.at[rows, :], a_sem.at[i])

    @pl.loop(0, blocks)
    def _(i):
        fetch(i).start()

    if packed:
        unpack_kernel(rem, n_vars, x_ref, h, hb.at[0])
    else:
        @pl.loop(0, blocks)
        def _(i):
            here = pl.ds(pl.multiple_of(i * block, block), block)
            h[:, here] = x_ref[:, here]
            hb[0, :, here] = x_ref[:, here].astype(jnp.bfloat16)

    for n in range(layers):
        now, later = n % 2, (n + 1) % 2

        def mix(i):
            if n == 0:
                fetch(i).wait()
            rows = a_all[pl.ds(pl.multiple_of(i * block, block), block), :]
            return lax.dot_general(hb[now], rows, (((1,), (1,)), ((), ())), preferred_element_type=jnp.float32).astype(jnp.bfloat16)

        def update(i, mixed):
            here = pl.ds(pl.multiple_of(i * block, block), block)
            half = jnp.dot(wt_ref[n], mixed, preferred_element_type=jnp.float32)
            arg = half * (2 * GELU_C + (8 * GELU_C * 0.044715) * (half * half))
            act = half * jnp.tanh(arg) + half
            new = h[:, here] + jnp.dot(ut_ref[n], act.astype(jnp.bfloat16), preferred_element_type=jnp.float32)
            h[:, here] = new
            hb[later, :, here] = new.astype(jnp.bfloat16)

        def body(i, mixed):
            following = mix(i)
            update(i - 1, mixed)
            return following

        update(blocks - 1, lax.fori_loop(1, blocks, body, mix(0)))
    pack_kernel(rem, h, o_ref)


def forecast(x, mix_op, wt, ut, n_blocks, block=BLOCK):
    cols = mix_op.shape[0]
    layers, n_vars, hidden = ut.shape
    rem = cols // n_blocks - LANES
    return pl.pallas_call(
        functools.partial(forecast_kernel, rem, x.ndim == 3, block),
        out_shape=jax.ShapeDtypeStruct((n_blocks, n_vars + n_vars * rem // LANES, LANES), jnp.float32),
        in_specs=[VMEM, pl.BlockSpec(memory_space=pl.ANY), VMEM, VMEM],
        out_specs=VMEM,
        scratch_shapes=[
            pltpu.VMEM(mix_op.shape, mix_op.dtype),
            pltpu.VMEM((n_vars, cols), jnp.float32),
            pltpu.VMEM((2, n_vars, cols), jnp.bfloat16),
            pltpu.SemaphoreType.DMA((cols // block,)),
        ],
        compiler_params=pltpu.CompilerParams(vmem_limit_bytes=VMEM_LIMIT),
        cost_estimate=pl.CostEstimate(flops=2 * layers * n_vars * cols * (cols + 2 * hidden), bytes_accessed=2 * cols * cols, transcendentals=layers * hidden * cols),
        name='forecast',
    )(x, mix_op, wt, ut)


def analysis_kernel(n_model, by_output, idx_ref, rho_ref, x_ref, y_ref, r_ref, o_ref, main, rest, pair, out_main, out_rest):
    xa, mean, yo, gy, vec, mats = main
    rxa, rmean, ryo, rgy, rvec, pieces = rest
    t_all, n_all = pair
    n_vars, deep = mean.shape[0], rmean.shape[0]
    n_obs = y_ref.shape[1]
    fold = n_vars // deep
    rem = LANES // fold
    depth = n_vars + deep
    members = x_ref.shape[0] // depth
    groups = members // SUB
    eight = lax.broadcasted_iota(jnp.int32, (SUB, LANES), 0)
    lane_group = lambda rows: lax.broadcasted_iota(jnp.int32, (rows, LANES), 1) // rem
    own_row = lax.broadcasted_iota(jnp.int32, (members, LANES), 0) - SUB * lane_group(members)
    total_eye = (members - 1) / rho_ref[0]

    def spread(x):
        shift = rem
        while shift < LANES:
            x = x + pltpu.roll(x, shift, 1)
            shift *= 2
        return x

    def turns(x):
        return [x] + [pltpu.roll(x, rem * g, 1) for g in range(1, fold)]

    def copies(turned, q):
        away = lax.rem(lane_group(turned[0].shape[0]) + (fold - q), fold)
        out = turned[0]
        for g in range(1, fold):
            out = jnp.where(away == g, turned[g], out)
        return out

    for first, rows, center, mean_ref in ((0, n_vars, xa, mean), (n_vars, deep, rxa, rmean)):
        total = x_ref[first:first + rows, :]
        for k in range(1, members):
            total = total + x_ref[k * depth + first:k * depth + first + rows, :]
        mean_ref[...] = total * (1.0 / members)

        @pl.loop(0, rows // 4)
        def _(v4):
            for c in range(4):
                v = v4 * 4 + c
                center[pl.ds(pl.multiple_of(v * members, SUB), members), :] = x_ref[pl.ds(v + first, members, stride=depth), :] - mean_ref[pl.ds(v, 1), :]

    @pl.loop(0, n_obs // 4)
    def _(p4):
        for c in range(4):
            p = p4 * 4 + c
            var = idx_ref[p]
            row = pl.multiple_of(p * members, SUB)
            here = xa[pl.ds(pl.multiple_of(var * members, SUB), members), :]
            yo[pl.ds(row, members), :] = here
            gy[pl.ds(row, members), :] = here * r_ref[0, pl.ds(p, 1), :]
            vec[pl.ds(p, 1), :] = y_ref[0, pl.ds(p, 1), :] - mean[pl.ds(var, 1), :]
            q, v = var // deep, lax.rem(var, deep)
            here = copies(turns(rxa[pl.ds(pl.multiple_of(v * members, SUB), members), :]), q)
            ryo[pl.ds(row, members), :] = here
            rgy[pl.ds(row, members), :] = here * r_ref[1, pl.ds(p, 1), :]
            level = copies(turns(jnp.broadcast_to(rmean[pl.ds(v, 1), :], (SUB, LANES))), q)
            rvec[pl.ds(p, 1), :] = y_ref[1, pl.ds(p, 1), :] - level[0:1]

    def product(left, left_at, right, right_at, out, out_at, scale=None, diag=None, mirror=True):
        plain = left is gy
        left_row = lambda k, i, a: k * members + SUB * i + a if plain or k < SUB * (i + 1) else (SUB * i + a) * members + k
        for blocks in PASSES:
            def body(kk, acc):
                acc = list(acc)
                for c in range(members):
                    row = c * members
                    for n, i in enumerate(blocks):
                        r = right[pl.ds(pl.multiple_of(right_at + row + SUB * i, SUB), members - SUB * i), :]
                        for a in range(SUB):
                            acc[n * SUB + a] = acc[n * SUB + a] + left[pl.ds(left_at + left_row(c, i, a), 1), :] * r
                return tuple(acc)

            start = [jnp.zeros((members - SUB * i, LANES), jnp.float32) for i in blocks for a in range(SUB)]
            acc = lax.fori_loop(0, 1, body, tuple(start))
            for n, i in enumerate(blocks):
                for a in range(SUB):
                    val = acc[n * SUB + a]
                    val = val if scale is None else val * scale
                    first = val[0:SUB] if diag is None else val[0:SUB] + jnp.where(eight == a, diag, 0.0)
                    row = (SUB * i + a) * members + SUB * i
                    out[pl.ds(pl.multiple_of(out_at + row, SUB), SUB), :] = first
                    if i + 1 < groups:
                        out[pl.ds(pl.multiple_of(out_at + row + SUB, SUB), members - SUB * (i + 1)), :] = val[SUB:]
                        if mirror:
                            out[pl.ds(out_at + SUB * (i + 1) * members + SUB * i + a, members - SUB * (i + 1), stride=members), :] = val[SUB:]


    def split_product(left, left_at, at, depth_k, right, out, out_at, scale=None, diag=None):
        def body(k8, acc):
            for c in range(8):
                k = k8 * 8 + c
                r = right[pl.ds(pl.multiple_of(k * members, SUB), members), :]
                acc = tuple(acc[a] + left[pl.ds(left_at + at(k, a), 1), :] * r for a in range(SUB))
            return acc

        acc = lax.fori_loop(0, depth_k // 8, body, tuple(jnp.zeros((members, LANES), jnp.float32) for a in range(SUB)))
        for a in range(SUB):
            val = acc[a] if scale is None else acc[a] * scale
            out[pl.ds(pl.multiple_of(out_at + a * members, SUB), members), :] = val if diag is None else val + jnp.where(own_row == a, diag, 0.0)

    def copy_all(split, split_at, out):
        @pl.loop(0, SUB // 2)
        def _(a2):
            for c in range(2):
                a = a2 * 2 + c
                turned = turns(split[pl.ds(pl.multiple_of(split_at + a * members, SUB), members), :])
                for q in range(fold):
                    out[pl.ds(pl.multiple_of((SUB * q + a) * members, SUB), members), :] = copies(turned, q)

    by_row = lambda k, a: a * members + k
    square, part = members * members, SUB * members
    slot = lambda n: lax.rem(n + 4 * NS_STEPS, 4)
    whole = lambda n: pl.multiple_of(slot(n) * square, SUB)
    piece = lambda n: pl.multiple_of(slot(n) * part, SUB)

    product(gy, 0, yo, 0, mats, 3 * square, None, total_eye)
    trace = jnp.sum(mats[pl.ds(3 * square, members, stride=members + 1), :], axis=0, keepdims=True)
    inv = 1.0 / trace

    @pl.loop(0, members)
    def _(i):
        row = pl.multiple_of(i * members, SUB)
        bi = mats[pl.ds(3 * square + row, members), :] * inv
        ti = jnp.where(lax.broadcasted_iota(jnp.int32, (members, LANES), 0) == i, 1.5, 0.0) - 0.5 * bi
        mats[pl.ds(row, members), :] = bi
        mats[pl.ds(square + row, members), :] = ti
        mats[pl.ds(2 * square + row, members), :] = ti

    @pl.loop(0, n_obs)
    def _(p):
        x = rgy[pl.ds(pl.multiple_of(p * members, SUB), members), :]
        half = x[0:SUB]
        for q in range(1, fold):
            half = jnp.where(lane_group(SUB) == q, x[SUB * q:SUB * (q + 1)], half)
        n_all[pl.ds(pl.multiple_of(p * SUB, SUB), SUB), :] = half

    split_product(n_all, 0, lambda k, a: k * SUB + a, n_obs, ryo, pieces, 3 * part, None, total_eye)
    rtrace = jnp.zeros((members, LANES), jnp.float32)
    for a in range(SUB):
        rtrace = rtrace + jnp.where(own_row == a, pieces[3 * part + a * members:3 * part + (a + 1) * members, :], 0.0)
    rtrace = spread(jnp.broadcast_to(jnp.sum(rtrace, axis=0, keepdims=True), (SUB, LANES)))[0:1]
    rinv = 1.0 / rtrace
    for a in range(SUB):
        here = slice(a * members, (a + 1) * members)
        bi = pieces[3 * part + a * members:3 * part + (a + 1) * members, :] * rinv
        ti = jnp.where(own_row == a, 1.5, 0.0) - 0.5 * bi
        pieces[a * members:(a + 1) * members, :] = bi
        pieces[part + a * members:part + (a + 1) * members, :] = ti
        pieces[2 * part + a * members:2 * part + (a + 1) * members, :] = ti
    copy_all(pieces, part, t_all)

    @pl.loop(0, NS_STEPS - 1)
    def _(s):
        b, t, z, n = whole(-s), whole(1 - s), whole(2 - s), whole(3 - s)
        rb, rt, rz, rn = piece(-s), piece(1 - s), piece(2 - s), piece(3 - s)
        product(mats, b, mats, t, mats, n)
        split_product(pieces, rb, by_row, members, t_all, pieces, rn)
        copy_all(pieces, rn, n_all)
        product(mats, z, mats, n, mats, b, -0.5, 1.5)
        split_product(pieces, rz, by_row, members, n_all, pieces, rb, -0.5, 1.5)
        copy_all(pieces, rb, t_all)
        product(mats, z, mats, b, mats, t, mirror=False)
        split_product(pieces, rz, by_row, members, t_all, pieces, rt)

    last = 3 - NS_STEPS
    for i in range(groups - 1):
        for a in range(SUB):
            val = mats[pl.ds(whole(last) + (SUB * i + a) * members + SUB * (i + 1), members - SUB * (i + 1)), :]
            mats[pl.ds(whole(last) + SUB * (i + 1) * members + SUB * i + a, members - SUB * (i + 1), stride=members), :] = val
    copy_all(pieces, piece(last), n_all)

    def finish(zs, at, trace, gy, vec, mean, xa, put):
        root = 1.0 / jnp.sqrt(trace)

        def weighted(left, left_at, base, count):
            acc = jnp.zeros((members, LANES), jnp.float32)
            for p in range(count):
                acc = acc + left[pl.ds(left_at + p * members, members), :] * vec[base + p:base + p + 1, :]
            return acc

        vec[n_obs:n_obs + members, :] = weighted(gy, 0, 0, n_obs)
        vec[n_obs + members:n_obs + 2 * members, :] = weighted(zs, at, n_obs, members) * root
        vec[n_obs:n_obs + members, :] = weighted(zs, at, n_obs + members, members) * root

        @pl.loop(0, members)
        def _(i):
            row = pl.multiple_of(i * members, SUB)
            gy[pl.ds(row, members), :] = zs[pl.ds(at + row, members), :] * (root * (members - 1) ** 0.5) + vec[pl.ds(n_obs + i, 1), :]

        @pl.loop(0, mean.shape[0] // 4)
        def _(v4):
            acc = [jnp.broadcast_to(mean[pl.ds(v4 * 4 + c, 1), :], (members, LANES)) for c in range(4)]
            for i in range(members):
                wa = gy[i * members:(i + 1) * members, :]
                acc = [acc[c] + xa[pl.ds((v4 * 4 + c) * members + i, 1), :] * wa for c in range(4)]
            for c in range(4):
                put(v4 * 4 + c, acc[c])

    if not by_output:
        def put(first):
            def store(v, val):
                o_ref[pl.ds(v + first, members, stride=depth), :] = val
            return store

        finish(mats, whole(last), trace, gy, vec, mean, xa, put(0))
        finish(n_all, 0, rtrace, rgy, rvec, rmean, rxa, put(n_vars))
        return

    def put(ref, rows):
        def store(v, val):
            ref[pl.ds(v, members, stride=rows), :] = val
        return store

    finish(mats, whole(last), trace, gy, vec, mean, xa, put(out_main, n_vars))
    finish(n_all, 0, rtrace, rgy, rvec, rmean, rxa, put(out_rest, deep))

    @pl.loop(0, members // n_model)
    def _(e):
        for m in range(n_model):
            row = (e * n_model + m) * depth
            for i in range(n_model):
                k = e * n_model + i
                o_ref[pl.ds(pl.multiple_of(row + deep * i, SUB), deep), :] = out_main[pl.ds(pl.multiple_of(k * n_vars + m * deep, SUB), deep), :]
                x = out_rest[pl.ds(pl.multiple_of(k * deep, SUB), deep), :]
                x = x if i == m else pltpu.roll(x, (rem * (i - m)) % LANES, 1)
                tail = x if i == 0 else jnp.where(lane_group(deep) == i, x, tail)
            o_ref[pl.ds(pl.multiple_of(row + n_vars, SUB), deep), :] = tail


def analysis(x, y, r, obs_idx, inflation, n_vars, n_model, by_output):
    members, depth, _ = x.shape
    n_obs = y.shape[1]
    deep = depth - n_vars
    rows = lambda n: pltpu.VMEM((n, LANES), jnp.float32)
    square, split = members * members, SUB * members
    both = [rows(n_obs * members), rows(n_obs * members), rows(n_obs + 2 * members)]
    return pl.pallas_call(
        functools.partial(analysis_kernel, n_model, by_output),
        out_shape=jax.ShapeDtypeStruct((members * depth, LANES), jnp.float32),
        in_specs=[SMEM, SMEM, VMEM, VMEM, VMEM],
        out_specs=VMEM,
        scratch_shapes=[
            [rows(n_vars * members), rows(n_vars)] + both + [rows(4 * square)],
            [rows(deep * members), rows(deep)] + both + [rows(4 * split)],
            [rows(square), rows(square)],
            rows(members * n_vars if by_output else SUB),
            rows(members * deep if by_output else SUB),
        ],
        name='analysis',
    )(obs_idx, inflation, x.reshape(members * depth, LANES), y, r).reshape(x.shape)


def by_lanes(x):
    x = jnp.swapaxes(x, -1, -2)
    rest = x[..., LANES:]
    rest = jnp.concatenate([rest] * (LANES // rest.shape[-1]), axis=-1)
    return jnp.stack([x[..., :LANES], rest], axis=-3)


def solution(mesh):
    n_model, n_ens = mesh.shape['model'], mesh.shape['ens']

    def local_step(ens_local, mix_op, w_in, w_out, obs_val, obs_prec, obs_idx, inflation):
        held, cols, own_vars = ens_local.shape
        n_blocks = n_model * n_ens
        cycles, layers, n_vars = obs_val.shape[0], w_in.shape[0], w_in.shape[1]
        x = jnp.swapaxes(ens_local, 1, 2)
        h, w_all, u_all = gather_vars(x, w_in, jnp.swapaxes(w_out, 1, 2), n_model)
        h = h.reshape(n_vars, cols)
        wt = (jnp.transpose(w_all, (1, 0, 3, 2)) * jnp.bfloat16(0.5)).reshape(layers, -1, n_vars)
        ut = jnp.transpose(u_all, (1, 2, 0, 3)).reshape(layers, n_vars, -1)
        y = by_lanes(obs_val)
        r = by_lanes(obs_prec)
        x = h
        for cycle in range(cycles):
            last = cycle + 1 == cycles
            x = exchange(forecast(x, mix_op, wt, ut, n_blocks), n_model, n_ens)
            x = analysis(x, y[cycle], r, obs_idx, inflation, n_vars, n_model, last)
            x = exchange(x, n_model, n_ens)
        (h,) = unpack(x, n_vars, (jnp.float32,))
        return jnp.swapaxes(h.reshape(held, own_vars, cols), 1, 2)

    member_spec = P(('case', 'ens'), None, 'model')
    col_axes = ('case', 'ens', 'model')
    in_specs = (member_spec, P(None, None), P(None, None, 'model'), P(None, 'model', None), P(None, col_axes, None), P(col_axes, None), P(None), P(None))
    return jax.shard_map(local_step, mesh=mesh, in_specs=in_specs, out_specs=member_spec, check_vma=False)
```

```python
import functools

import jax
import jax.numpy as jnp
from jax import lax
from jax.experimental import pallas as pl
from jax.experimental.pallas import tpu as pltpu
from jax.sharding import PartitionSpec as P

NS_STEPS = 12
UNROLL = 16
PASSES = ((0,), (1,), (2, 3))
LANES = 128
BLOCK = 512
TALL = (True,)
VMEM_LIMIT = 66_500_000
GELU_C = 0.7978845608028654
SUB = 8
MESH = pl.DeviceIdType.MESH
VMEM = pl.BlockSpec(memory_space=pltpu.VMEM)
HBM = pl.BlockSpec(memory_space=pl.ANY)
SMEM = pl.BlockSpec(memory_space=pltpu.SMEM)


def greet(peers):
    barrier = pltpu.get_barrier_semaphore()
    for peer in peers:
        pl.semaphore_signal(barrier, inc=1, device_id=peer, device_id_type=MESH)
    pl.semaphore_wait(barrier, len(peers))


def gather_vars_kernel(n_model, x_ref, w_ref, u_ref, h_ref, wa_ref, ua_ref, send_sem, recv_sem, own_sem):
    me = lax.axis_index('model')
    others = [lax.rem(me + t, n_model) for t in range(1, n_model)]
    greet([{'model': o} for o in others])
    copies = []
    for t, o in enumerate(others):
        for a, (src, dst) in enumerate(((x_ref.at[o], h_ref.at[me]), (w_ref, wa_ref.at[me]), (u_ref, ua_ref.at[me]))):
            copies.append(pltpu.make_async_remote_copy(src_ref=src, dst_ref=dst, send_sem=send_sem.at[3 * t + a], recv_sem=recv_sem.at[3 * t + a], device_id={'model': o}, device_id_type=MESH))
    for copy in copies:
        copy.start()
    own = [pltpu.make_async_copy(src, dst, own_sem.at[a]) for a, (src, dst) in enumerate(((x_ref.at[me], h_ref.at[me]), (w_ref, wa_ref.at[me]), (u_ref, ua_ref.at[me])))]
    for copy in own:
        copy.start()
    for copy in own + copies:
        copy.wait()


def gather_vars(x, w, u, n_model):
    n_sem = 3 * (n_model - 1)
    return pl.pallas_call(
        functools.partial(gather_vars_kernel, n_model),
        out_shape=(jax.ShapeDtypeStruct(x.shape, x.dtype), jax.ShapeDtypeStruct((n_model,) + w.shape, w.dtype), jax.ShapeDtypeStruct((n_model,) + u.shape, u.dtype)),
        in_specs=[VMEM] * 3,
        out_specs=[VMEM] * 3,
        scratch_shapes=[pltpu.SemaphoreType.DMA((n_sem,)), pltpu.SemaphoreType.DMA((n_sem,)), pltpu.SemaphoreType.DMA((3,))],
        compiler_params=pltpu.CompilerParams(collective_id=0, has_side_effects=True),
        name='gather_vars',
    )(x, w, u)


def exchange_kernel(n_model, n_ens, x_ref, o_ref, send_sem, recv_sem, own_sem):
    my_m, my_e = lax.axis_index('model'), lax.axis_index('ens')
    me = my_e * n_model + my_m
    steps = [(e, m) for e in range(n_ens) for m in range(n_model)][1:]
    peers = [(lax.rem(my_e + e, n_ens), lax.rem(my_m + m, n_model)) for e, m in steps]
    greet([{'ens': e, 'model': m} for e, m in peers])
    copies = []
    for t, (e, m) in enumerate(peers):
        copies.append(pltpu.make_async_remote_copy(src_ref=x_ref.at[e * n_model + m], dst_ref=o_ref.at[me], send_sem=send_sem.at[t], recv_sem=recv_sem.at[t], device_id={'ens': e, 'model': m}, device_id_type=MESH))
    for copy in copies:
        copy.start()
    own = pltpu.make_async_copy(x_ref.at[me], o_ref.at[me], own_sem)
    own.start()
    own.wait()
    for copy in copies:
        copy.wait()


def exchange(x, n_model, n_ens):
    n_sem = n_model * n_ens - 1
    return pl.pallas_call(
        functools.partial(exchange_kernel, n_model, n_ens),
        out_shape=jax.ShapeDtypeStruct(x.shape, x.dtype),
        in_specs=[HBM],
        out_specs=HBM,
        scratch_shapes=[pltpu.SemaphoreType.DMA((n_sem,)), pltpu.SemaphoreType.DMA((n_sem,)), pltpu.SemaphoreType.DMA],
        compiler_params=pltpu.CompilerParams(collective_id=1, has_side_effects=True),
        name='exchange',
    )(x)


def lane_pick(lanes, pieces):
    out = pieces[-1][1]
    for bound, piece in reversed(pieces[:-1]):
        out = jnp.where(lanes < bound, piece, out)
    return out


def pack_kernel(rem, h_ref, o_ref):
    fold = LANES // rem
    rows = h_ref.shape[0]
    deep = rows // fold
    span = fold * (LANES + rem)
    lanes = lax.broadcasted_iota(jnp.int32, (rows, LANES), 1)
    dlanes = lax.broadcasted_iota(jnp.int32, (deep, LANES), 1)

    @pl.loop(0, h_ref.shape[1] // span)
    def _(a):
        part = [h_ref[:, pl.ds(pl.multiple_of(a * span + g * LANES, LANES), LANES)] for g in range(fold + 1)]
        for b in range(fold):
            j = a * fold + b
            main = part[0] if b == 0 else pltpu.roll(jnp.where(lanes < rem * b, part[b + 1], part[b]), LANES - rem * b, 1)
            o_ref[j, 0:rows, :] = main
            tail = [part[b + 1][deep * q:deep * (q + 1)] for q in range(fold)]
            tail = [x if q == b else pltpu.roll(x, (rem * (q - b)) % LANES, 1) for q, x in enumerate(tail)]
            o_ref[j, rows:rows + deep, :] = lane_pick(dlanes, [(rem * (q + 1), x) for q, x in enumerate(tail)])


def unpack_kernel(rem, rows, x_ref, *outs):
    fold = LANES // rem
    deep = rows // fold
    span = fold * (LANES + rem)
    lanes = lax.broadcasted_iota(jnp.int32, (rows, LANES), 1)

    @pl.loop(0, x_ref.shape[0] // fold)
    def _(a):
        mains, tails = [], []
        for b in range(fold):
            main = x_ref[a * fold + b, 0:rows, :]
            mains.append(main if b == 0 else pltpu.roll(main, rem * b, 1))
            tail = x_ref[a * fold + b, rows:rows + deep, :]
            tails.append(jnp.concatenate([tail if q == b else pltpu.roll(tail, (rem * (b - q)) % LANES, 1) for q in range(fold)], axis=0))
        for g in range(fold + 1):
            if g == 0:
                piece = mains[0]
            else:
                piece = jnp.where(lanes < rem * (g - 1), mains[g - 1], tails[g - 1])
                if g < fold:
                    piece = jnp.where(lanes < rem * g, piece, mains[g])
            for out in outs:
                out[:, pl.ds(pl.multiple_of(a * span + g * LANES, LANES), LANES)] = piece.astype(out.dtype)


def unpack(x, rows, dtypes):
    n_blocks, depth, _ = x.shape
    rem = (depth - rows) * LANES // rows
    return pl.pallas_call(
        functools.partial(unpack_kernel, rem, rows),
        out_shape=tuple(jax.ShapeDtypeStruct((rows, n_blocks * (LANES + rem)), t) for t in dtypes),
        in_specs=[VMEM],
        out_specs=tuple(VMEM for t in dtypes),
        name='unpack',
    )(x)


def forecast_kernel(rem, packed, block, x_ref, a_ref, wt_ref, ut_ref, o_ref, a_all, h, hb, a_sem):
    layers = wt_ref.shape[0]
    n_vars, cols = h.shape
    blocks = cols // block

    def fetch(i):
        rows = pl.ds(pl.multiple_of(i * block, block), block)
        return pltpu.make_async_copy(a_ref.at[rows, :], a_all.at[rows, :], a_sem.at[i])

    @pl.loop(0, blocks)
    def _(i):
        fetch(i).start()

    if packed:
        unpack_kernel(rem, n_vars, x_ref, h, hb.at[0])
    else:
        @pl.loop(0, blocks)
        def _(i):
            here = pl.ds(pl.multiple_of(i * block, block), block)
            h[:, here] = x_ref[:, here]
            hb[0, :, here] = x_ref[:, here].astype(jnp.bfloat16)

    for n in range(layers):
        now, later = n % 2, (n + 1) % 2

        def mix(i):
            out = []
            for j, tall in enumerate(TALL):
                if n == 0:
                    fetch(i * len(TALL) + j).wait()
                rows = a_all[pl.ds(pl.multiple_of((i * len(TALL) + j) * block, block), block), :]
                pair = (rows, hb[now]) if tall else (hb[now], rows)
                out.append(lax.dot_general(*pair, (((1,), (1,)), ((), ())), preferred_element_type=jnp.float32).astype(jnp.bfloat16))
            return tuple(out)

        def update(i, mixed):
            for j, tall in enumerate(TALL):
                here = pl.ds(pl.multiple_of((i * len(TALL) + j) * block, block), block)
                half = lax.dot_general(wt_ref[n], mixed[j], (((1,), (1 if tall else 0,)), ((), ())), preferred_element_type=jnp.float32)
                arg = half * (2 * GELU_C + (8 * GELU_C * 0.044715) * (half * half))
                act = half * jnp.tanh(arg) + half
                new = h[:, here] + jnp.dot(ut_ref[n], act.astype(jnp.bfloat16), preferred_element_type=jnp.float32)
                h[:, here] = new
                hb[later, :, here] = new.astype(jnp.bfloat16)

        def body(i, mixed):
            following = mix(i)
            update(i - 1, mixed)
            return following

        steps = blocks // len(TALL)
        update(steps - 1, lax.fori_loop(1, steps, body, mix(0)))
    pack_kernel(rem, h, o_ref)


def forecast(x, mix_op, wt, ut, n_blocks, block=BLOCK):
    cols = mix_op.shape[0]
    layers, n_vars, hidden = ut.shape
    rem = cols // n_blocks - LANES
    return pl.pallas_call(
        functools.partial(forecast_kernel, rem, x.ndim == 3, block),
        out_shape=jax.ShapeDtypeStruct((n_blocks, n_vars + n_vars * rem // LANES, LANES), jnp.float32),
        in_specs=[VMEM, pl.BlockSpec(memory_space=pl.ANY), VMEM, VMEM],
        out_specs=VMEM,
        scratch_shapes=[
            pltpu.VMEM(mix_op.shape, mix_op.dtype),
            pltpu.VMEM((n_vars, cols), jnp.float32),
            pltpu.VMEM((2, n_vars, cols), jnp.bfloat16),
            pltpu.SemaphoreType.DMA((cols // block,)),
        ],
        compiler_params=pltpu.CompilerParams(vmem_limit_bytes=VMEM_LIMIT),
        cost_estimate=pl.CostEstimate(flops=2 * layers * n_vars * cols * (cols + 2 * hidden), bytes_accessed=2 * cols * cols, transcendentals=layers * hidden * cols),
        name='forecast',
    )(x, mix_op, wt, ut)


def analysis_kernel(n_model, by_output, idx_ref, rho_ref, x_ref, y_ref, r_ref, o_ref, main, rest, pair, out_main, out_rest):
    xa, mean, yo, gy, vec, mats = main
    rxa, rmean, ryo, rgy, rvec, pieces = rest
    t_all, n_all = pair
    n_vars, deep = mean.shape[0], rmean.shape[0]
    n_obs = y_ref.shape[1]
    fold = n_vars // deep
    rem = LANES // fold
    depth = n_vars + deep
    members = x_ref.shape[0] // depth
    groups = members // SUB
    eight = lax.broadcasted_iota(jnp.int32, (SUB, LANES), 0)
    lane_group = lambda rows: lax.broadcasted_iota(jnp.int32, (rows, LANES), 1) // rem
    own_row = lax.broadcasted_iota(jnp.int32, (members, LANES), 0) - SUB * lane_group(members)
    total_eye = (members - 1) / rho_ref[0]

    def spread(x):
        shift = rem
        while shift < LANES:
            x = x + pltpu.roll(x, shift, 1)
            shift *= 2
        return x

    def turns(x):
        return [x] + [pltpu.roll(x, rem * g, 1) for g in range(1, fold)]

    def copies(turned, q):
        away = lax.rem(lane_group(turned[0].shape[0]) + (fold - q), fold)
        out = turned[0]
        for g in range(1, fold):
            out = jnp.where(away == g, turned[g], out)
        return out

    for first, rows, center, mean_ref in ((0, n_vars, xa, mean), (n_vars, deep, rxa, rmean)):
        total = x_ref[first:first + rows, :]
        for k in range(1, members):
            total = total + x_ref[k * depth + first:k * depth + first + rows, :]
        mean_ref[...] = total * (1.0 / members)

        @pl.loop(0, rows // 4)
        def _(v4):
            for c in range(4):
                v = v4 * 4 + c
                center[pl.ds(pl.multiple_of(v * members, SUB), members), :] = x_ref[pl.ds(v + first, members, stride=depth), :] - mean_ref[pl.ds(v, 1), :]

    @pl.loop(0, n_obs // 4)
    def _(p4):
        for c in range(4):
            p = p4 * 4 + c
            var = idx_ref[p]
            row = pl.multiple_of(p * members, SUB)
            here = xa[pl.ds(pl.multiple_of(var * members, SUB), members), :]
            yo[pl.ds(row, members), :] = here
            gy[pl.ds(row, members), :] = here * r_ref[0, pl.ds(p, 1), :]
            vec[pl.ds(p, 1), :] = y_ref[0, pl.ds(p, 1), :] - mean[pl.ds(var, 1), :]
            q, v = var // deep, lax.rem(var, deep)
            here = copies(turns(rxa[pl.ds(pl.multiple_of(v * members, SUB), members), :]), q)
            ryo[pl.ds(row, members), :] = here
            rgy[pl.ds(row, members), :] = here * r_ref[1, pl.ds(p, 1), :]
            level = copies(turns(jnp.broadcast_to(rmean[pl.ds(v, 1), :], (SUB, LANES))), q)
            rvec[pl.ds(p, 1), :] = y_ref[1, pl.ds(p, 1), :] - level[0:1]

    def product(left, left_at, right, right_at, out, out_at, scale=None, diag=None, mirror=True):
        plain = left is gy
        left_row = lambda k, i, a: k * members + SUB * i + a
        for blocks in PASSES:
            def body(kk, acc):
                acc = list(acc)
                for c in range(UNROLL):
                    row = (kk * UNROLL + c) * members
                    for n, i in enumerate(blocks):
                        r = right[pl.ds(pl.multiple_of(right_at + row + SUB * i, SUB), members - SUB * i), :]
                        for a in range(SUB):
                            acc[n * SUB + a] = acc[n * SUB + a] + left[pl.ds(left_at + left_row(kk * UNROLL + c, i, a), 1), :] * r
                return tuple(acc)

            start = [jnp.zeros((members - SUB * i, LANES), jnp.float32) for i in blocks for a in range(SUB)]
            acc = lax.fori_loop(0, members // UNROLL, body, tuple(start))
            for n, i in enumerate(blocks):
                for a in range(SUB):
                    val = acc[n * SUB + a]
                    val = val if scale is None else val * scale
                    first = val[0:SUB] if diag is None else val[0:SUB] + jnp.where(eight == a, diag, 0.0)
                    row = (SUB * i + a) * members + SUB * i
                    out[pl.ds(pl.multiple_of(out_at + row, SUB), SUB), :] = first
                    if i + 1 < groups:
                        out[pl.ds(pl.multiple_of(out_at + row + SUB, SUB), members - SUB * (i + 1)), :] = val[SUB:]
                        if mirror:
                            out[pl.ds(out_at + SUB * (i + 1) * members + SUB * i + a, members - SUB * (i + 1), stride=members), :] = val[SUB:]


    def split_product(left, left_at, at, depth_k, right, out, out_at, scale=None, diag=None):
        def body(k8, acc):
            for c in range(8):
                k = k8 * 8 + c
                r = right[pl.ds(pl.multiple_of(k * members, SUB), members), :]
                acc = tuple(acc[a] + left[pl.ds(left_at + at(k, a), 1), :] * r for a in range(SUB))
            return acc

        acc = lax.fori_loop(0, depth_k // 8, body, tuple(jnp.zeros((members, LANES), jnp.float32) for a in range(SUB)))
        for a in range(SUB):
            val = acc[a] if scale is None else acc[a] * scale
            out[pl.ds(pl.multiple_of(out_at + a * members, SUB), members), :] = val if diag is None else val + jnp.where(own_row == a, diag, 0.0)

    def copy_all(split, split_at, out):
        @pl.loop(0, SUB // 2)
        def _(a2):
            for c in range(2):
                a = a2 * 2 + c
                turned = turns(split[pl.ds(pl.multiple_of(split_at + a * members, SUB), members), :])
                for q in range(fold):
                    out[pl.ds(pl.multiple_of((SUB * q + a) * members, SUB), members), :] = copies(turned, q)

    by_row = lambda k, a: a * members + k
    square, part = members * members, SUB * members
    at_p, at_s, at_v, at_f, at_b, at_z = range(6)

    product(gy, 0, yo, 0, mats, at_s * square, None, total_eye)
    trace = jnp.sum(mats[pl.ds(at_s * square, members, stride=members + 1), :], axis=0, keepdims=True)
    inv = 1.0 / trace

    @pl.loop(0, members)
    def _(i):
        row = pl.multiple_of(i * members, SUB)
        bi = mats[pl.ds(at_s * square + row, members), :] * inv
        mats[pl.ds(at_p * square + row, members), :] = bi
        mats[pl.ds(at_b * square + row, members), :] = bi
        mats[pl.ds(at_z * square + row, members), :] = jnp.where(lax.broadcasted_iota(jnp.int32, (members, LANES), 0) == i, 1.0, 0.0)

    @pl.loop(0, n_obs)
    def _(p):
        x = rgy[pl.ds(pl.multiple_of(p * members, SUB), members), :]
        half = x[0:SUB]
        for q in range(1, fold):
            half = jnp.where(lane_group(SUB) == q, x[SUB * q:SUB * (q + 1)], half)
        n_all[pl.ds(pl.multiple_of(p * SUB, SUB), SUB), :] = half

    split_product(n_all, 0, lambda k, a: k * SUB + a, n_obs, ryo, pieces, at_s * part, None, total_eye)
    rtrace = jnp.zeros((members, LANES), jnp.float32)
    for a in range(SUB):
        rtrace = rtrace + jnp.where(own_row == a, pieces[at_s * part + a * members:at_s * part + (a + 1) * members, :], 0.0)
    rtrace = spread(jnp.broadcast_to(jnp.sum(rtrace, axis=0, keepdims=True), (SUB, LANES)))[0:1]
    rinv = 1.0 / rtrace
    for a in range(SUB):
        row = a * members
        bi = pieces[at_s * part + row:at_s * part + row + members, :] * rinv
        pieces[at_p * part + row:at_p * part + row + members, :] = bi
        pieces[at_b * part + row:at_b * part + row + members, :] = bi
        pieces[at_z * part + row:at_z * part + row + members, :] = jnp.where(own_row == a, 1.0, 0.0)

    def combine(out, diag, p, x):
        to, of = out

        @pl.loop(0, members // 4)
        def _(i4):
            for c in range(4):
                i = i4 * 4 + c
                row = pl.multiple_of(i * members, SUB)
                eye = jnp.where(lax.broadcasted_iota(jnp.int32, (members, LANES), 0) == i, diag, 0.0)
                mats[pl.ds(to * square + row, members), :] = eye + p * mats[pl.ds(at_p * square + row, members), :] + x * mats[pl.ds(of * square + row, members), :]
        for a in range(SUB):
            row = a * members
            eye = jnp.where(own_row == a, diag, 0.0)
            pieces[to * part + row:to * part + row + members, :] = eye + p * pieces[at_p * part + row:at_p * part + row + members, :] + x * pieces[of * part + row:of * part + row + members, :]

    def both(left, right, out, copied, mirror=True):
        product(mats, left * square, mats, right * square, mats, out * square, mirror=mirror)
        split_product(pieces, left * part, by_row, members, copied, pieces, out * part)

    def move(of, to):
        @pl.loop(0, SUB)
        def _(a):
            here = members * groups
            mats[pl.ds(pl.multiple_of(to * square + a * here, SUB), here), :] = mats[pl.ds(pl.multiple_of(of * square + a * here, SUB), here), :]
            pieces[pl.ds(pl.multiple_of(to * part + a * members, SUB), members), :] = pieces[pl.ds(pl.multiple_of(of * part + a * members, SUB), members), :]

    @pl.loop(0, NS_STEPS // 2)
    def _(s):
        copy_all(pieces, at_p * part, n_all)
        both(at_p, at_p, at_s, n_all)
        combine((at_v, at_s), 27.0, -9.0, 1.0)
        copy_all(pieces, at_s * part, n_all)
        both(at_v, at_s, at_f, n_all)
        combine((at_f, at_f), 36.0 / 16, -39.0 / 16, 1.0 / 16)
        copy_all(pieces, at_f * part, t_all)
        both(at_z, at_f, at_s, t_all)
        move(at_s, at_z)

        @pl.when(s + 1 < NS_STEPS // 2)
        def _():
            both(at_b, at_f, at_v, t_all)
            copy_all(pieces, at_v * part, n_all)
            both(at_z, at_v, at_p, n_all)
            move(at_v, at_b)

    z_row = at_z * square
    for i in range(groups - 1):
        for a in range(SUB):
            val = mats[pl.ds(z_row + (SUB * i + a) * members + SUB * (i + 1), members - SUB * (i + 1)), :]
            mats[pl.ds(z_row + SUB * (i + 1) * members + SUB * i + a, members - SUB * (i + 1), stride=members), :] = val
    copy_all(pieces, at_z * part, n_all)

    def finish(zs, at, trace, gy, vec, mean, xa, put):
        root = 1.0 / jnp.sqrt(trace)

        def weighted(left, left_at, base, count):
            acc = jnp.zeros((members, LANES), jnp.float32)
            for p in range(count):
                acc = acc + left[pl.ds(left_at + p * members, members), :] * vec[base + p:base + p + 1, :]
            return acc

        vec[n_obs:n_obs + members, :] = weighted(gy, 0, 0, n_obs)
        vec[n_obs + members:n_obs + 2 * members, :] = weighted(zs, at, n_obs, members) * root
        vec[n_obs:n_obs + members, :] = weighted(zs, at, n_obs + members, members) * root

        @pl.loop(0, members)
        def _(i):
            row = pl.multiple_of(i * members, SUB)
            gy[pl.ds(row, members), :] = zs[pl.ds(at + row, members), :] * (root * (members - 1) ** 0.5) + vec[pl.ds(n_obs + i, 1), :]

        @pl.loop(0, mean.shape[0] // 4)
        def _(v4):
            acc = [jnp.broadcast_to(mean[pl.ds(v4 * 4 + c, 1), :], (members, LANES)) for c in range(4)]
            for i in range(members):
                wa = gy[i * members:(i + 1) * members, :]
                acc = [acc[c] + xa[pl.ds((v4 * 4 + c) * members + i, 1), :] * wa for c in range(4)]
            for c in range(4):
                put(v4 * 4 + c, acc[c])

    if not by_output:
        def put(first):
            def store(v, val):
                o_ref[pl.ds(v + first, members, stride=depth), :] = val
            return store

        finish(mats, z_row, trace, gy, vec, mean, xa, put(0))
        finish(n_all, 0, rtrace, rgy, rvec, rmean, rxa, put(n_vars))
        return

    def put(ref, rows):
        def store(v, val):
            ref[pl.ds(v, members, stride=rows), :] = val
        return store

    finish(mats, z_row, trace, gy, vec, mean, xa, put(out_main, n_vars))
    finish(n_all, 0, rtrace, rgy, rvec, rmean, rxa, put(out_rest, deep))

    @pl.loop(0, members // n_model)
    def _(e):
        for m in range(n_model):
            row = (e * n_model + m) * depth
            for i in range(n_model):
                k = e * n_model + i
                o_ref[pl.ds(pl.multiple_of(row + deep * i, SUB), deep), :] = out_main[pl.ds(pl.multiple_of(k * n_vars + m * deep, SUB), deep), :]
                x = out_rest[pl.ds(pl.multiple_of(k * deep, SUB), deep), :]
                x = x if i == m else pltpu.roll(x, (rem * (i - m)) % LANES, 1)
                tail = x if i == 0 else jnp.where(lane_group(deep) == i, x, tail)
            o_ref[pl.ds(pl.multiple_of(row + n_vars, SUB), deep), :] = tail


def analysis(x, y, r, obs_idx, inflation, n_vars, n_model, by_output):
    members, depth, _ = x.shape
    n_obs = y.shape[1]
    deep = depth - n_vars
    rows = lambda n: pltpu.VMEM((n, LANES), jnp.float32)
    square, split = members * members, SUB * members
    both = [rows(n_obs * members), rows(n_obs * members), rows(n_obs + 2 * members)]
    return pl.pallas_call(
        functools.partial(analysis_kernel, n_model, by_output),
        out_shape=jax.ShapeDtypeStruct((members * depth, LANES), jnp.float32),
        in_specs=[SMEM, SMEM, VMEM, VMEM, VMEM],
        out_specs=VMEM,
        scratch_shapes=[
            [rows(n_vars * members), rows(n_vars)] + both + [rows(6 * square)],
            [rows(deep * members), rows(deep)] + both + [rows(6 * split)],
            [rows(square), rows(square)],
            rows(members * n_vars if by_output else SUB),
            rows(members * deep if by_output else SUB),
        ],
        name='analysis',
    )(obs_idx, inflation, x.reshape(members * depth, LANES), y, r).reshape(x.shape)


def by_lanes(x):
    x = jnp.swapaxes(x, -1, -2)
    rest = x[..., LANES:]
    rest = jnp.concatenate([rest] * (LANES // rest.shape[-1]), axis=-1)
    return jnp.stack([x[..., :LANES], rest], axis=-3)


def solution(mesh):
    n_model, n_ens = mesh.shape['model'], mesh.shape['ens']

    def local_step(ens_local, mix_op, w_in, w_out, obs_val, obs_prec, obs_idx, inflation):
        held, cols, own_vars = ens_local.shape
        n_blocks = n_model * n_ens
        cycles, layers, n_vars = obs_val.shape[0], w_in.shape[0], w_in.shape[1]
        x = jnp.swapaxes(ens_local, 1, 2)
        h, w_all, u_all = gather_vars(x, w_in, jnp.swapaxes(w_out, 1, 2), n_model)
        h = h.reshape(n_vars, cols)
        wt = (jnp.transpose(w_all, (1, 0, 3, 2)) * jnp.bfloat16(0.5)).reshape(layers, -1, n_vars)
        ut = jnp.transpose(u_all, (1, 2, 0, 3)).reshape(layers, n_vars, -1)
        y = by_lanes(obs_val)
        r = by_lanes(obs_prec)
        x = h
        for cycle in range(cycles):
            last = cycle + 1 == cycles
            x = exchange(forecast(x, mix_op, wt, ut, n_blocks), n_model, n_ens)
            x = analysis(x, y[cycle], r, obs_idx, inflation, n_vars, n_model, last)
            x = exchange(x, n_model, n_ens)
        (h,) = unpack(x, n_vars, (jnp.float32,))
        return jnp.swapaxes(h.reshape(held, own_vars, cols), 1, 2)

    member_spec = P(('case', 'ens'), None, 'model')
    col_axes = ('case', 'ens', 'model')
    in_specs = (member_spec, P(None, None), P(None, None, 'model'), P(None, 'model', None), P(None, col_axes, None), P(col_axes, None), P(None), P(None))
    return jax.shard_map(local_step, mesh=mesh, in_specs=in_specs, out_specs=member_spec, check_vma=False)
```

```python
import functools

import jax
import jax.numpy as jnp
from jax import lax
from jax.experimental import pallas as pl
from jax.experimental.pallas import tpu as pltpu
from jax.sharding import PartitionSpec as P

NS_STEPS = 12
UNROLL = 16
PASSES = ((0,), (1,), (2, 3))
LANES = 128
BLOCK = 512
TALL = (True,)
VMEM_LIMIT = 66_500_000
GELU_C = 0.7978845608028654
SUB = 8
MESH = pl.DeviceIdType.MESH
VMEM = pl.BlockSpec(memory_space=pltpu.VMEM)
HBM = pl.BlockSpec(memory_space=pl.ANY)
SMEM = pl.BlockSpec(memory_space=pltpu.SMEM)


def greet(peers):
    barrier = pltpu.get_barrier_semaphore()
    for peer in peers:
        pl.semaphore_signal(barrier, inc=1, device_id=peer, device_id_type=MESH)
    pl.semaphore_wait(barrier, len(peers))


def gather_vars_kernel(n_model, n_ens, x_ref, w_ref, h_ref, wa_ref, send_sem, recv_sem, own_sem):
    me, mine = lax.axis_index('model'), lax.axis_index('ens')
    tiles = w_ref.shape[0] // n_ens
    part = pl.ds(mine * tiles, tiles)
    around = [lax.rem(me + t, n_model) for t in range(1, n_model)]
    along = [lax.rem(mine + t, n_ens) for t in range(1, n_ens)]
    greet([{'model': o} for o in around] + [{'ens': o} for o in along])
    count = iter(range(send_sem.shape[0]))

    def remote(src, dst, where):
        i = next(count)
        return pltpu.make_async_remote_copy(src_ref=src, dst_ref=dst, send_sem=send_sem.at[i], recv_sem=recv_sem.at[i], device_id=where, device_id_type=MESH)

    shards = [remote(w_ref.at[part], wa_ref.at[me, part], {'model': o}) for o in around]
    members = [remote(x_ref.at[o], h_ref.at[me], {'model': o}) for o in around]
    for copy in shards + members:
        copy.start()
    own = [pltpu.make_async_copy(x_ref.at[me], h_ref.at[me], own_sem.at[0]), pltpu.make_async_copy(w_ref, wa_ref.at[me], own_sem.at[1])]
    for copy in own:
        copy.start()
    for copy in shards:
        copy.wait()
    onward = [remote(wa_ref.at[s, part], wa_ref.at[s, part], {'ens': o}) for o in along for s in around]
    for copy in onward:
        copy.start()
    for copy in own + members + onward:
        copy.wait()


def gather_vars(x, w, n_model, n_ens):
    n_sem = (n_model - 1) * (n_ens + 1)
    return pl.pallas_call(
        functools.partial(gather_vars_kernel, n_model, n_ens),
        out_shape=(jax.ShapeDtypeStruct(x.shape, x.dtype), jax.ShapeDtypeStruct((n_model,) + w.shape, w.dtype)),
        in_specs=[VMEM] * 2,
        out_specs=[VMEM] * 2,
        scratch_shapes=[pltpu.SemaphoreType.DMA((n_sem,)), pltpu.SemaphoreType.DMA((n_sem,)), pltpu.SemaphoreType.DMA((2,))],
        compiler_params=pltpu.CompilerParams(collective_id=0, has_side_effects=True),
        name='gather_vars',
    )(x, w)


def exchange_kernel(n_model, n_ens, x_ref, o_ref, send_sem, recv_sem, own_sem):
    my_m, my_e = lax.axis_index('model'), lax.axis_index('ens')
    me = my_e * n_model + my_m
    steps = [(e, m) for e in range(n_ens) for m in range(n_model)][1:]
    peers = [(lax.rem(my_e + e, n_ens), lax.rem(my_m + m, n_model)) for e, m in steps]
    greet([{'ens': e, 'model': m} for e, m in peers])
    copies = []
    for t, (e, m) in enumerate(peers):
        copies.append(pltpu.make_async_remote_copy(src_ref=x_ref.at[e * n_model + m], dst_ref=o_ref.at[me], send_sem=send_sem.at[t], recv_sem=recv_sem.at[t], device_id={'ens': e, 'model': m}, device_id_type=MESH))
    for copy in copies:
        copy.start()
    own = pltpu.make_async_copy(x_ref.at[me], o_ref.at[me], own_sem)
    own.start()
    own.wait()
    for copy in copies:
        copy.wait()


def exchange(x, n_model, n_ens):
    n_sem = n_model * n_ens - 1
    return pl.pallas_call(
        functools.partial(exchange_kernel, n_model, n_ens),
        out_shape=jax.ShapeDtypeStruct(x.shape, x.dtype),
        in_specs=[HBM],
        out_specs=HBM,
        scratch_shapes=[pltpu.SemaphoreType.DMA((n_sem,)), pltpu.SemaphoreType.DMA((n_sem,)), pltpu.SemaphoreType.DMA],
        compiler_params=pltpu.CompilerParams(collective_id=1, has_side_effects=True),
        name='exchange',
    )(x)


def lane_pick(lanes, pieces):
    out = pieces[-1][1]
    for bound, piece in reversed(pieces[:-1]):
        out = jnp.where(lanes < bound, piece, out)
    return out


def pack_kernel(rem, h_ref, o_ref):
    fold = LANES // rem
    rows = h_ref.shape[0]
    deep = rows // fold
    span = fold * (LANES + rem)
    lanes = lax.broadcasted_iota(jnp.int32, (rows, LANES), 1)
    dlanes = lax.broadcasted_iota(jnp.int32, (deep, LANES), 1)

    @pl.loop(0, h_ref.shape[1] // span)
    def _(a):
        part = [h_ref[:, pl.ds(pl.multiple_of(a * span + g * LANES, LANES), LANES)] for g in range(fold + 1)]
        for b in range(fold):
            j = a * fold + b
            main = part[0] if b == 0 else pltpu.roll(jnp.where(lanes < rem * b, part[b + 1], part[b]), LANES - rem * b, 1)
            o_ref[j, 0:rows, :] = main
            tail = [part[b + 1][deep * q:deep * (q + 1)] for q in range(fold)]
            tail = [x if q == b else pltpu.roll(x, (rem * (q - b)) % LANES, 1) for q, x in enumerate(tail)]
            o_ref[j, rows:rows + deep, :] = lane_pick(dlanes, [(rem * (q + 1), x) for q, x in enumerate(tail)])


def unpack_kernel(rem, rows, x_ref, *outs):
    fold = LANES // rem
    deep = rows // fold
    span = fold * (LANES + rem)
    lanes = lax.broadcasted_iota(jnp.int32, (rows, LANES), 1)

    @pl.loop(0, x_ref.shape[0] // fold)
    def _(a):
        mains, tails = [], []
        for b in range(fold):
            main = x_ref[a * fold + b, 0:rows, :]
            mains.append(main if b == 0 else pltpu.roll(main, rem * b, 1))
            tail = x_ref[a * fold + b, rows:rows + deep, :]
            tails.append(jnp.concatenate([tail if q == b else pltpu.roll(tail, (rem * (b - q)) % LANES, 1) for q in range(fold)], axis=0))
        for g in range(fold + 1):
            if g == 0:
                piece = mains[0]
            else:
                piece = jnp.where(lanes < rem * (g - 1), mains[g - 1], tails[g - 1])
                if g < fold:
                    piece = jnp.where(lanes < rem * g, piece, mains[g])
            for out in outs:
                out[:, pl.ds(pl.multiple_of(a * span + g * LANES, LANES), LANES)] = piece.astype(out.dtype)


def unpack(x, rows, dtypes):
    n_blocks, depth, _ = x.shape
    rem = (depth - rows) * LANES // rows
    return pl.pallas_call(
        functools.partial(unpack_kernel, rem, rows),
        out_shape=tuple(jax.ShapeDtypeStruct((rows, n_blocks * (LANES + rem)), t) for t in dtypes),
        in_specs=[VMEM],
        out_specs=tuple(VMEM for t in dtypes),
        name='unpack',
    )(x)


def forecast_kernel(rem, packed, block, x_ref, a_ref, wt_ref, ut_ref, o_ref, a_all, h, hb, a_sem):
    layers = wt_ref.shape[0]
    n_vars, cols = h.shape
    blocks = cols // block

    def fetch(i):
        rows = pl.ds(pl.multiple_of(i * block, block), block)
        return pltpu.make_async_copy(a_ref.at[rows, :], a_all.at[rows, :], a_sem.at[i])

    @pl.loop(0, blocks)
    def _(i):
        fetch(i).start()

    if packed:
        unpack_kernel(rem, n_vars, x_ref, h, hb.at[0])
    else:
        @pl.loop(0, blocks)
        def _(i):
            here = pl.ds(pl.multiple_of(i * block, block), block)
            h[:, here] = x_ref[:, here]
            hb[0, :, here] = x_ref[:, here].astype(jnp.bfloat16)

    for n in range(layers):
        now, later = n % 2, (n + 1) % 2

        def mix(i):
            out = []
            for j, tall in enumerate(TALL):
                if n == 0:
                    fetch(i * len(TALL) + j).wait()
                rows = a_all[pl.ds(pl.multiple_of((i * len(TALL) + j) * block, block), block), :]
                pair = (rows, hb[now]) if tall else (hb[now], rows)
                out.append(lax.dot_general(*pair, (((1,), (1,)), ((), ())), preferred_element_type=jnp.float32).astype(jnp.bfloat16))
            return tuple(out)

        def update(i, mixed):
            for j, tall in enumerate(TALL):
                here = pl.ds(pl.multiple_of((i * len(TALL) + j) * block, block), block)
                half = lax.dot_general(wt_ref[n], mixed[j], (((1,), (1 if tall else 0,)), ((), ())), preferred_element_type=jnp.float32)
                arg = half * (2 * GELU_C + (8 * GELU_C * 0.044715) * (half * half))
                act = half * jnp.tanh(arg) + half
                new = h[:, here] + jnp.dot(ut_ref[n], act.astype(jnp.bfloat16), preferred_element_type=jnp.float32)
                h[:, here] = new
                hb[later, :, here] = new.astype(jnp.bfloat16)

        def body(i, mixed):
            following = mix(i)
            update(i - 1, mixed)
            return following

        steps = blocks // len(TALL)
        update(steps - 1, lax.fori_loop(1, steps, body, mix(0)))
    pack_kernel(rem, h, o_ref)


def forecast(x, mix_op, wt, ut, n_blocks, block=BLOCK):
    cols = mix_op.shape[0]
    layers, n_vars, hidden = ut.shape
    rem = cols // n_blocks - LANES
    return pl.pallas_call(
        functools.partial(forecast_kernel, rem, x.ndim == 3, block),
        out_shape=jax.ShapeDtypeStruct((n_blocks, n_vars + n_vars * rem // LANES, LANES), jnp.float32),
        in_specs=[VMEM, pl.BlockSpec(memory_space=pl.ANY), VMEM, VMEM],
        out_specs=VMEM,
        scratch_shapes=[
            pltpu.VMEM(mix_op.shape, mix_op.dtype),
            pltpu.VMEM((n_vars, cols), jnp.float32),
            pltpu.VMEM((2, n_vars, cols), jnp.bfloat16),
            pltpu.SemaphoreType.DMA((cols // block,)),
        ],
        compiler_params=pltpu.CompilerParams(vmem_limit_bytes=VMEM_LIMIT),
        cost_estimate=pl.CostEstimate(flops=2 * layers * n_vars * cols * (cols + 2 * hidden), bytes_accessed=2 * cols * cols, transcendentals=layers * hidden * cols),
        name='forecast',
    )(x, mix_op, wt, ut)


def analysis_kernel(n_model, by_output, idx_ref, rho_ref, x_ref, y_ref, r_ref, o_ref, main, rest, pair, out_main, out_rest):
    xa, mean, yo, gy, vec, mats = main
    rxa, rmean, ryo, rgy, rvec, pieces = rest
    t_all, n_all = pair
    n_vars, deep = mean.shape[0], rmean.shape[0]
    n_obs = y_ref.shape[1]
    fold = n_vars // deep
    rem = LANES // fold
    depth = n_vars + deep
    members = x_ref.shape[0] // depth
    groups = members // SUB
    eight = lax.broadcasted_iota(jnp.int32, (SUB, LANES), 0)
    lane_group = lambda rows: lax.broadcasted_iota(jnp.int32, (rows, LANES), 1) // rem
    own_row = lax.broadcasted_iota(jnp.int32, (members, LANES), 0) - SUB * lane_group(members)
    total_eye = (members - 1) / rho_ref[0]

    def spread(x):
        shift = rem
        while shift < LANES:
            x = x + pltpu.roll(x, shift, 1)
            shift *= 2
        return x

    def turns(x):
        return [x] + [pltpu.roll(x, rem * g, 1) for g in range(1, fold)]

    def copies(turned, q):
        away = lax.rem(lane_group(turned[0].shape[0]) + (fold - q), fold)
        out = turned[0]
        for g in range(1, fold):
            out = jnp.where(away == g, turned[g], out)
        return out

    for first, rows, center, mean_ref in ((0, n_vars, xa, mean), (n_vars, deep, rxa, rmean)):
        total = x_ref[first:first + rows, :]
        for k in range(1, members):
            total = total + x_ref[k * depth + first:k * depth + first + rows, :]
        mean_ref[...] = total * (1.0 / members)

        @pl.loop(0, rows // 4)
        def _(v4):
            for c in range(4):
                v = v4 * 4 + c
                center[pl.ds(pl.multiple_of(v * members, SUB), members), :] = x_ref[pl.ds(v + first, members, stride=depth), :] - mean_ref[pl.ds(v, 1), :]

    @pl.loop(0, n_obs // 4)
    def _(p4):
        for c in range(4):
            p = p4 * 4 + c
            var = idx_ref[p]
            row = pl.multiple_of(p * members, SUB)
            here = xa[pl.ds(pl.multiple_of(var * members, SUB), members), :]
            yo[pl.ds(row, members), :] = here
            gy[pl.ds(row, members), :] = here * r_ref[0, pl.ds(p, 1), :]
            vec[pl.ds(p, 1), :] = y_ref[0, pl.ds(p, 1), :] - mean[pl.ds(var, 1), :]
            q, v = var // deep, lax.rem(var, deep)
            here = copies(turns(rxa[pl.ds(pl.multiple_of(v * members, SUB), members), :]), q)
            ryo[pl.ds(row, members), :] = here
            rgy[pl.ds(row, members), :] = here * r_ref[1, pl.ds(p, 1), :]
            level = copies(turns(jnp.broadcast_to(rmean[pl.ds(v, 1), :], (SUB, LANES))), q)
            rvec[pl.ds(p, 1), :] = y_ref[1, pl.ds(p, 1), :] - level[0:1]

    def product(left, left_at, right, right_at, out, out_at, scale=None, diag=None, mirror=True):
        plain = left is gy
        left_row = lambda k, i, a: k * members + SUB * i + a
        for blocks in PASSES:
            def body(kk, acc):
                acc = list(acc)
                for c in range(UNROLL):
                    row = (kk * UNROLL + c) * members
                    for n, i in enumerate(blocks):
                        r = right[pl.ds(pl.multiple_of(right_at + row + SUB * i, SUB), members - SUB * i), :]
                        for a in range(SUB):
                            acc[n * SUB + a] = acc[n * SUB + a] + left[pl.ds(left_at + left_row(kk * UNROLL + c, i, a), 1), :] * r
                return tuple(acc)

            start = [jnp.zeros((members - SUB * i, LANES), jnp.float32) for i in blocks for a in range(SUB)]
            acc = lax.fori_loop(0, members // UNROLL, body, tuple(start))
            for n, i in enumerate(blocks):
                for a in range(SUB):
                    val = acc[n * SUB + a]
                    val = val if scale is None else val * scale
                    first = val[0:SUB] if diag is None else val[0:SUB] + jnp.where(eight == a, diag, 0.0)
                    row = (SUB * i + a) * members + SUB * i
                    out[pl.ds(pl.multiple_of(out_at + row, SUB), SUB), :] = first
                    if i + 1 < groups:
                        out[pl.ds(pl.multiple_of(out_at + row + SUB, SUB), members - SUB * (i + 1)), :] = val[SUB:]
                        if mirror:
                            out[pl.ds(out_at + SUB * (i + 1) * members + SUB * i + a, members - SUB * (i + 1), stride=members), :] = val[SUB:]


    def split_product(left, left_at, at, depth_k, right, out, out_at, scale=None, diag=None):
        def body(k8, acc):
            for c in range(8):
                k = k8 * 8 + c
                r = right[pl.ds(pl.multiple_of(k * members, SUB), members), :]
                acc = tuple(acc[a] + left[pl.ds(left_at + at(k, a), 1), :] * r for a in range(SUB))
            return acc

        acc = lax.fori_loop(0, depth_k // 8, body, tuple(jnp.zeros((members, LANES), jnp.float32) for a in range(SUB)))
        for a in range(SUB):
            val = acc[a] if scale is None else acc[a] * scale
            out[pl.ds(pl.multiple_of(out_at + a * members, SUB), members), :] = val if diag is None else val + jnp.where(own_row == a, diag, 0.0)

    def copy_all(split, split_at, out):
        @pl.loop(0, SUB // 2)
        def _(a2):
            for c in range(2):
                a = a2 * 2 + c
                turned = turns(split[pl.ds(pl.multiple_of(split_at + a * members, SUB), members), :])
                for q in range(fold):
                    out[pl.ds(pl.multiple_of((SUB * q + a) * members, SUB), members), :] = copies(turned, q)

    by_row = lambda k, a: a * members + k
    square, part = members * members, SUB * members
    at_p, at_s, at_v, at_f, at_b, at_z = range(6)

    product(gy, 0, yo, 0, mats, at_s * square, None, total_eye)
    trace = jnp.sum(mats[pl.ds(at_s * square, members, stride=members + 1), :], axis=0, keepdims=True)
    inv = 1.0 / trace

    @pl.loop(0, members)
    def _(i):
        row = pl.multiple_of(i * members, SUB)
        bi = mats[pl.ds(at_s * square + row, members), :] * inv
        mats[pl.ds(at_p * square + row, members), :] = bi
        mats[pl.ds(at_b * square + row, members), :] = bi
        mats[pl.ds(at_z * square + row, members), :] = jnp.where(lax.broadcasted_iota(jnp.int32, (members, LANES), 0) == i, 1.0, 0.0)

    @pl.loop(0, n_obs)
    def _(p):
        x = rgy[pl.ds(pl.multiple_of(p * members, SUB), members), :]
        half = x[0:SUB]
        for q in range(1, fold):
            half = jnp.where(lane_group(SUB) == q, x[SUB * q:SUB * (q + 1)], half)
        n_all[pl.ds(pl.multiple_of(p * SUB, SUB), SUB), :] = half

    split_product(n_all, 0, lambda k, a: k * SUB + a, n_obs, ryo, pieces, at_s * part, None, total_eye)
    rtrace = jnp.zeros((members, LANES), jnp.float32)
    for a in range(SUB):
        rtrace = rtrace + jnp.where(own_row == a, pieces[at_s * part + a * members:at_s * part + (a + 1) * members, :], 0.0)
    rtrace = spread(jnp.broadcast_to(jnp.sum(rtrace, axis=0, keepdims=True), (SUB, LANES)))[0:1]
    rinv = 1.0 / rtrace
    for a in range(SUB):
        row = a * members
        bi = pieces[at_s * part + row:at_s * part + row + members, :] * rinv
        pieces[at_p * part + row:at_p * part + row + members, :] = bi
        pieces[at_b * part + row:at_b * part + row + members, :] = bi
        pieces[at_z * part + row:at_z * part + row + members, :] = jnp.where(own_row == a, 1.0, 0.0)

    def combine(out, diag, p, x):
        to, of = out

        @pl.loop(0, members // 4)
        def _(i4):
            for c in range(4):
                i = i4 * 4 + c
                row = pl.multiple_of(i * members, SUB)
                eye = jnp.where(lax.broadcasted_iota(jnp.int32, (members, LANES), 0) == i, diag, 0.0)
                mats[pl.ds(to * square + row, members), :] = eye + p * mats[pl.ds(at_p * square + row, members), :] + x * mats[pl.ds(of * square + row, members), :]
        for a in range(SUB):
            row = a * members
            eye = jnp.where(own_row == a, diag, 0.0)
            pieces[to * part + row:to * part + row + members, :] = eye + p * pieces[at_p * part + row:at_p * part + row + members, :] + x * pieces[of * part + row:of * part + row + members, :]

    def both(left, right, out, copied, mirror=True):
        product(mats, left * square, mats, right * square, mats, out * square, mirror=mirror)
        split_product(pieces, left * part, by_row, members, copied, pieces, out * part)

    def move(of, to):
        @pl.loop(0, SUB)
        def _(a):
            here = members * groups
            mats[pl.ds(pl.multiple_of(to * square + a * here, SUB), here), :] = mats[pl.ds(pl.multiple_of(of * square + a * here, SUB), here), :]
            pieces[pl.ds(pl.multiple_of(to * part + a * members, SUB), members), :] = pieces[pl.ds(pl.multiple_of(of * part + a * members, SUB), members), :]

    @pl.loop(0, NS_STEPS // 2)
    def _(s):
        copy_all(pieces, at_p * part, n_all)
        both(at_p, at_p, at_s, n_all)
        combine((at_v, at_s), 27.0, -9.0, 1.0)
        copy_all(pieces, at_s * part, n_all)
        both(at_v, at_s, at_f, n_all)
        combine((at_f, at_f), 36.0 / 16, -39.0 / 16, 1.0 / 16)
        copy_all(pieces, at_f * part, t_all)
        both(at_z, at_f, at_s, t_all)
        move(at_s, at_z)

        @pl.when(s + 1 < NS_STEPS // 2)
        def _():
            both(at_b, at_f, at_v, t_all)
            copy_all(pieces, at_v * part, n_all)
            both(at_z, at_v, at_p, n_all)
            move(at_v, at_b)

    z_row = at_z * square
    for i in range(groups - 1):
        for a in range(SUB):
            val = mats[pl.ds(z_row + (SUB * i + a) * members + SUB * (i + 1), members - SUB * (i + 1)), :]
            mats[pl.ds(z_row + SUB * (i + 1) * members + SUB * i + a, members - SUB * (i + 1), stride=members), :] = val
    copy_all(pieces, at_z * part, n_all)

    def finish(zs, at, trace, gy, vec, mean, xa, put):
        root = 1.0 / jnp.sqrt(trace)

        def weighted(left, left_at, base, count):
            acc = jnp.zeros((members, LANES), jnp.float32)
            for p in range(count):
                acc = acc + left[pl.ds(left_at + p * members, members), :] * vec[base + p:base + p + 1, :]
            return acc

        vec[n_obs:n_obs + members, :] = weighted(gy, 0, 0, n_obs)
        vec[n_obs + members:n_obs + 2 * members, :] = weighted(zs, at, n_obs, members) * root
        vec[n_obs:n_obs + members, :] = weighted(zs, at, n_obs + members, members) * root

        @pl.loop(0, members)
        def _(i):
            row = pl.multiple_of(i * members, SUB)
            gy[pl.ds(row, members), :] = zs[pl.ds(at + row, members), :] * (root * (members - 1) ** 0.5) + vec[pl.ds(n_obs + i, 1), :]

        @pl.loop(0, mean.shape[0] // 4)
        def _(v4):
            acc = [jnp.broadcast_to(mean[pl.ds(v4 * 4 + c, 1), :], (members, LANES)) for c in range(4)]
            for i in range(members):
                wa = gy[i * members:(i + 1) * members, :]
                acc = [acc[c] + xa[pl.ds((v4 * 4 + c) * members + i, 1), :] * wa for c in range(4)]
            for c in range(4):
                put(v4 * 4 + c, acc[c])

    if not by_output:
        def put(first):
            def store(v, val):
                o_ref[pl.ds(v + first, members, stride=depth), :] = val
            return store

        finish(mats, z_row, trace, gy, vec, mean, xa, put(0))
        finish(n_all, 0, rtrace, rgy, rvec, rmean, rxa, put(n_vars))
        return

    def put(ref, rows):
        def store(v, val):
            ref[pl.ds(v, members, stride=rows), :] = val
        return store

    finish(mats, z_row, trace, gy, vec, mean, xa, put(out_main, n_vars))
    finish(n_all, 0, rtrace, rgy, rvec, rmean, rxa, put(out_rest, deep))

    @pl.loop(0, members // n_model)
    def _(e):
        for m in range(n_model):
            row = (e * n_model + m) * depth
            for i in range(n_model):
                k = e * n_model + i
                o_ref[pl.ds(pl.multiple_of(row + deep * i, SUB), deep), :] = out_main[pl.ds(pl.multiple_of(k * n_vars + m * deep, SUB), deep), :]
                x = out_rest[pl.ds(pl.multiple_of(k * deep, SUB), deep), :]
                x = x if i == m else pltpu.roll(x, (rem * (i - m)) % LANES, 1)
                tail = x if i == 0 else jnp.where(lane_group(deep) == i, x, tail)
            o_ref[pl.ds(pl.multiple_of(row + n_vars, SUB), deep), :] = tail


def analysis(x, y, r, obs_idx, inflation, n_vars, n_model, by_output):
    members, depth, _ = x.shape
    n_obs = y.shape[1]
    deep = depth - n_vars
    rows = lambda n: pltpu.VMEM((n, LANES), jnp.float32)
    square, split = members * members, SUB * members
    both = [rows(n_obs * members), rows(n_obs * members), rows(n_obs + 2 * members)]
    return pl.pallas_call(
        functools.partial(analysis_kernel, n_model, by_output),
        out_shape=jax.ShapeDtypeStruct((members * depth, LANES), jnp.float32),
        in_specs=[SMEM, SMEM, VMEM, VMEM, VMEM],
        out_specs=VMEM,
        scratch_shapes=[
            [rows(n_vars * members), rows(n_vars)] + both + [rows(6 * square)],
            [rows(deep * members), rows(deep)] + both + [rows(6 * split)],
            [rows(square), rows(square)],
            rows(members * n_vars if by_output else SUB),
            rows(members * deep if by_output else SUB),
        ],
        name='analysis',
    )(obs_idx, inflation, x.reshape(members * depth, LANES), y, r).reshape(x.shape)


def by_lanes(x):
    x = jnp.swapaxes(x, -1, -2)
    rest = x[..., LANES:]
    rest = jnp.concatenate([rest] * (LANES // rest.shape[-1]), axis=-1)
    return jnp.stack([x[..., :LANES], rest], axis=-3)


def solution(mesh):
    n_model, n_ens = mesh.shape['model'], mesh.shape['ens']

    def local_step(ens_local, mix_op, w_in, w_out, obs_val, obs_prec, obs_idx, inflation):
        held, cols, own_vars = ens_local.shape
        n_blocks = n_model * n_ens
        cycles, layers, n_vars = obs_val.shape[0], w_in.shape[0], w_in.shape[1]
        x = jnp.swapaxes(ens_local, 1, 2)
        w_own = jnp.concatenate([w_in, jnp.swapaxes(w_out, 1, 2)])
        h, w_all = gather_vars(x, w_own.reshape(-1, 2 * SUB, w_own.shape[2]), n_model, n_ens)
        h = h.reshape(n_vars, cols)
        w_all = w_all.reshape((n_model,) + w_own.shape)
        wt = (jnp.transpose(w_all[:, :layers], (1, 0, 3, 2)) * jnp.bfloat16(0.5)).reshape(layers, -1, n_vars)
        ut = jnp.transpose(w_all[:, layers:], (1, 2, 0, 3)).reshape(layers, n_vars, -1)
        y = by_lanes(obs_val)
        r = by_lanes(obs_prec)
        x = h
        for cycle in range(cycles):
            last = cycle + 1 == cycles
            x = exchange(forecast(x, mix_op, wt, ut, n_blocks), n_model, n_ens)
            x = analysis(x, y[cycle], r, obs_idx, inflation, n_vars, n_model, last)
            x = exchange(x, n_model, n_ens)
        (h,) = unpack(x, n_vars, (jnp.float32,))
        return jnp.swapaxes(h.reshape(held, own_vars, cols), 1, 2)

    member_spec = P(('case', 'ens'), None, 'model')
    col_axes = ('case', 'ens', 'model')
    in_specs = (member_spec, P(None, None), P(None, None, 'model'), P(None, 'model', None), P(None, col_axes, None), P(col_axes, None), P(None), P(None))
    return jax.shard_map(local_step, mesh=mesh, in_specs=in_specs, out_specs=member_spec, check_vma=False)
```
